256 devices in a mesh: blk: 128 (over x, z, y_lo, core), mp: 2 (over y_hi).
Axes of the slice: x: 4, y: 4 (y_hi: 2, y_lo: 2; y = y_hi * 2 + y_lo), z: 8, core: 2. Of those that a mesh axis runs over, the one named last changes fastest.
Arguments:
- features: bfloat16 [128, 2, 2, 256, 1280], P('blk', None, None, None, 'mp'), may hold values from -62 to 62
- w_query: bfloat16 [1280, 1280], P(None, 'mp'), may hold values from -2 to 2
- w_key: bfloat16 [1280, 1280], P(None, 'mp'), may hold values from -2 to 2
- w_value: bfloat16 [1280, 1280], P(None, 'mp'), may hold values from -0.15625 to 0.15625
- w_out: bfloat16 [1280, 1280], P('mp'), may hold values from -0.15625 to 0.15625
- w_head: bfloat16 [1280, 64], replicated, may hold values from -0.15625 to 0.15625
- offsets: int32 [128], P('blk'), may hold values from 0 to 2047, as said below
- blend_mask: int32 [128, 64, 64], P('blk'), may hold values from 1 to 4
Outputs:
- panorama: float32 [2, 2048, 256], P(None, 'blk')
The draws below stay inside these ranges and needn't reach their ends.
Inputs may be any that keep to these rules, and one draw needn't show every extreme that they name: offsets[w] = 16 * w + s for one s shared by all windows, 0 <= s < 16.
All inputs are finite; a program needn't handle non-finite values.
Results may differ from the reference program's by a relative error of at most 0.0064.
Values may be sent and summed in bfloat16 or wider, within the bound.
A program may use at most 64 MiB of HBM per device.

```python
import jax
import jax.numpy as jnp
from jax import lax

D = 1280
HEADS = 20
HEAD = 64
BATCH = 2
GRID = 16
PATCH = 4
CHAN = 4
STRIDE = 16
TOK = 256
WINDOW = 64
LAT = 256
OUTW = 64
NWIN = 128
WIDTH = 2048


def draw_features(key, part):
    normal_draw = jnp.clip(jax.random.normal(jax.random.fold_in(key, 11), (NWIN, BATCH, 2, TOK, D), jnp.float32), -6.0, 6.0)
    return normal_draw.astype(jnp.bfloat16)


def head_weight(key, salt):
    normal_draw = jnp.clip(jax.random.normal(jax.random.fold_in(key, salt), (D, D), jnp.float32), -6.0, 6.0) / D ** 0.5
    normal_draw = jnp.clip(normal_draw, -2.0, 2.0)
    return normal_draw.astype(jnp.bfloat16)


def draw_w_query(key, part):
    return head_weight(key, 21)


def draw_w_key(key, part):
    return head_weight(key, 22)


def draw_offsets(key, part):
    shared = jax.random.randint(jax.random.fold_in(key, 31), (), 0, STRIDE, jnp.int32)
    return (STRIDE * jnp.arange(NWIN, dtype=jnp.int32) + shared).astype(jnp.int32)


def touch_ends(values, stream_key, low, high):
    place = [jax.random.randint(jax.random.fold_in(stream_key, axis), (), 0, length) for axis, length in enumerate(values.shape)]
    main_axis = values.shape.index(max(values.shape))
    neighbour = place[:main_axis] + [(place[main_axis] + 1) % values.shape[main_axis]] + place[main_axis + 1:]
    return values.at[tuple(place)].set(low).at[tuple(neighbour)].set(high)


def steps_of(own_key, shape, shards, low, top_value):
    factor_of, own = 1.0, jax.random.fold_in(own_key, 6)
    for axis_at, parts in shards:
        heights = jnp.exp(jax.random.uniform(jax.random.fold_in(own, axis_at), (parts,), jnp.float32, low / len(shards), top_value / len(shards)))
        factor_of = factor_of * jnp.repeat(heights, shape[axis_at] // parts).reshape([-1 if axis == axis_at else 1 for axis in range(len(shape))])
    return factor_of


def noise(own_key, shape, scale, most, split=(), held_as=jnp.bfloat16):
    result = scale * jax.random.normal(own_key, shape, jnp.float32)
    if split:
        result = result * steps_of(own_key, shape, split, -0.22, 0.18)
    return jnp.clip(result, -most, most).astype(held_as)


def setup_inputs(seed: int = 0) -> dict:
    key_of = jax.random.split(jax.random.key(seed), 9)
    return {
        "features": draw_features(jax.random.fold_in(key_of[8], 71), 0),
        "w_query": draw_w_query(jax.random.fold_in(key_of[8], 71), 0),
        "w_key": draw_w_key(jax.random.fold_in(key_of[8], 71), 0),
        "w_value": noise(key_of[3], (D, D), D ** -0.5, 0.15625, ((1, 2),)),
        "w_out": noise(key_of[4], (D, D), D ** -0.5, 0.15625, ((0, 2),)),
        "w_head": noise(key_of[5], (D, OUTW), D ** -0.5, 0.15625),
        "offsets": draw_offsets(jax.random.fold_in(key_of[8], 71), 0),
        "blend_mask": touch_ends(jax.random.randint(key_of[7], (NWIN, WINDOW, WINDOW), 1, 5), jax.random.fold_in(key_of[7], 1), 1, 4).astype(jnp.int32),
    }


guidance = 3.0

def window_eps(window_data, w_query, w_key, w_value, w_out, w_head):
    token_rows = window_data.reshape(-1, D).astype(jnp.float32)
    row_mean = lax.optimization_barrier(jnp.mean(token_rows, axis=1, keepdims=True))
    centred = token_rows - row_mean
    row_var = lax.optimization_barrier(jnp.mean(centred * centred, axis=1, keepdims=True))
    normed = (centred * lax.rsqrt(row_var + 1e-05)).astype(jnp.bfloat16)
    sequences = BATCH * 2
    queries = jnp.dot(normed, w_query, preferred_element_type=jnp.float32).astype(jnp.bfloat16).reshape(sequences, TOK, HEADS, HEAD)
    key_rows = jnp.dot(normed, w_key, preferred_element_type=jnp.float32).astype(jnp.bfloat16).reshape(sequences, TOK, HEADS, HEAD)
    value_rows = jnp.dot(normed, w_value, preferred_element_type=jnp.float32).astype(jnp.bfloat16).reshape(sequences, TOK, HEADS, HEAD)
    scores = jnp.einsum('sqhd,skhd->shqk', queries.astype(jnp.float32), key_rows.astype(jnp.float32)) / HEAD ** 0.5
    scores = scores - lax.optimization_barrier(jnp.max(scores, axis=3, keepdims=True))
    expont = jnp.exp(scores)
    attend = (expont / lax.optimization_barrier(jnp.sum(expont, axis=3, keepdims=True))).astype(jnp.bfloat16)
    context = jnp.einsum('shqk,skhd->sqhd', attend.astype(jnp.float32), value_rows.astype(jnp.float32)).astype(jnp.bfloat16).reshape(-1, D)
    attention = jnp.dot(context, w_out, preferred_element_type=jnp.float32)
    tok_out = jnp.dot(token_rows + attention, w_head.astype(jnp.float32), precision=lax.Precision.HIGHEST)
    tok_out = tok_out.reshape(BATCH, 2, TOK, OUTW)
    guided = tok_out[:, 0] + guidance * (tok_out[:, 1] - tok_out[:, 0])
    spread = guided.reshape(BATCH, GRID, GRID, PATCH, PATCH, CHAN).transpose(0, 2, 3, 1, 4, 5)
    return spread.reshape(BATCH, WINDOW, LAT)

def reference(features, w_query, w_key, w_value, w_out, w_head, offsets, blend_mask):

    def one_window(window_data):
        return window_eps(window_data, w_query, w_key, w_value, w_out, w_head)
    spread_all = lax.map(one_window, features)
    weight = blend_mask.astype(jnp.float32)
    weight_wide = jnp.repeat(weight, CHAN, axis=2)
    columns = ((offsets[:, None] + jnp.arange(WINDOW, dtype=jnp.int32)[None, :]) % WIDTH).astype(jnp.int32).reshape(-1)
    weighted = (spread_all * weight_wide[:, None]).transpose(1, 0, 2, 3).reshape(BATCH, NWIN * WINDOW, LAT)
    numerator = jnp.zeros((BATCH, WIDTH, LAT), jnp.float32).at[:, columns].add(weighted)
    weight_total = jnp.zeros((WIDTH, WINDOW), jnp.float32).at[columns].add(weight.reshape(-1, WINDOW))
    return numerator / jnp.repeat(weight_total, CHAN, axis=1)[None]
```

```python
import jax
import jax.numpy as jnp
from jax import lax
from jax.experimental import pallas as pl
from jax.experimental.pallas import tpu as pltpu
from jax.sharding import PartitionSpec as P

MESH = pl.DeviceIdType.MESH
F32 = jnp.float32
BF16 = jnp.bfloat16

D = 1280
HALF = 640
TOK = 256
OUTW = 64
STRIDE = 16
WINDOW = 64
LAT = 256
FRAME = WINDOW + STRIDE
PIECES = 5
XS, ZS = 4, 8
BLK = 128
ROWS = D // ZS
SLABS = 16
OWN, OTH = 0, 1
EXP_SCALE = 1.4426950408889634 / 8.0
GUIDANCE = 3.0


def iota(shape, dim):
    return lax.broadcasted_iota(jnp.int32, shape, dim)


def kernel(
    f_ref, wq_ref, wk_ref, wv_ref, wo_ref, wh_ref, offs_ref, mask_ref, out_ref,
    wbuf, wout, whead, whz, maskv, xin, nrm, qkv, ctx, acc, rep, fold, mstage, mrecv, ostage, orecv,
    ld_sem, s_sem, fx_sem, inj_sem, a1_sem, a2_sem, b1_sem, b2_sem, sib_sem, m_sem, o_sem, oself_sem,
):
    blk = lax.axis_index("blk")
    mp = lax.axis_index("mp")
    core = lax.rem(blk, 2)
    ylo = lax.rem(blk // 2, 2)
    z = lax.rem(blk // 4, ZS)
    x = blk // (4 * ZS)

    def at(xx, zz, yy, cc):
        return ((xx * ZS + zz) * 2 + yy) * 2 + cc

    def dev(b, m):
        return (b, m)

    def ring(v, k, n):
        return lax.rem(v + k + n, n)

    side = dev(at(x, z, 1 - ylo, core), mp)
    cross = dev(at(x, z, 1 - ylo, core), 1 - mp)
    xdev = [dev(at(ring(x, k, XS), z, ylo, core), mp) for k in (1, 2, 3)]
    zplus = dev(at(x, ring(z, 1, ZS), ylo, core), mp)
    zminus = dev(at(x, ring(z, -1, ZS), ylo, core), mp)
    sibling = dev(at(x, z, ylo, 1 - core), mp)
    window = blk + 2 - 4 * ylo

    def window_of(b):
        return b + 2 - 4 * lax.rem(b // 2, 2)

    loads = []

    def load(src, dst):
        copy = pltpu.make_async_copy(src, dst, ld_sem.at[len(loads)])
        copy.start()
        loads.append(copy)
        return copy

    ld_wo = load(wo_ref, wout)
    ld_wh = load(wh_ref, whead)
    ld_mask = load(mask_ref.at[0], maskv)
    ld_w = []
    for m, ref in enumerate((wq_ref, wk_ref, wv_ref)):
        for j in range(5):
            ld_w.append(load(ref.at[:, pl.ds(128 * j, 128)], wbuf.at[OWN, 5 * m + j]))

    barrier = pltpu.get_barrier_semaphore()

    def greet(d):
        pl.semaphore_signal(barrier, inc=1, device_id=d, device_id_type=MESH)

    for d in [side, cross, *xdev, zplus, zminus, sibling]:
        greet(d)
    for j in range(1, PIECES):
        greet(dev(ring(blk, j, BLK), mp))
        greet(dev(ring(blk, -j, BLK), mp))
    for j in range(PIECES):
        target = ring(window, j, BLK)
        source = window_of(ring(blk, -j, BLK))
        greet(dev(target, 1 - mp))
        greet(dev(source, 1 - mp))
        if j != 2:
            greet(dev(target, mp))
            greet(dev(source, mp))

    @pl.when(ylo == 0)
    def _():
        greet(dev(ring(window, 2, BLK), mp))
        greet(dev(window_of(ring(blk, -2, BLK)), mp))

    shift = offs_ref[0] - STRIDE * blk
    ld_wh.wait()
    lane = iota((1, 128), 1)
    low = lane < 64
    twice = jnp.concatenate([whead[...], whead[...]], axis=1)
    whz[...] = jnp.where(low, twice.astype(F32), 0.0).astype(BF16)
    ld_wo.wait()
    for r in range(0, HALF, 128):
        prod = jnp.dot(wout[r : r + 128, :], twice, preferred_element_type=F32)
        head = prod.astype(BF16).astype(F32)
        wbuf[OWN, 15, r : r + 128, :] = jnp.where(low, head, prod - head).astype(BF16)
        wbuf[OWN, 15, HALF + r : HALF + r + 128, :] = jnp.zeros((128, 128), BF16)

    ld_mask.wait()
    widen = (iota((WINDOW, LAT), 0) == (iota((WINDOW, LAT), 1) >> 2)).astype(F32).astype(BF16)
    wide = jnp.dot(maskv[...].astype(F32).astype(BF16), widen, preferred_element_type=F32)
    move = (iota((FRAME, WINDOW), 0) - iota((FRAME, WINDOW), 1) == shift).astype(F32).astype(BF16)
    mstage[...] = jnp.dot(move, wide.astype(BF16), preferred_element_type=F32)
    mrecv[0] = mstage[0:STRIDE, :]

    for copy in ld_w:
        copy.wait()
    pl.semaphore_wait(barrier, 34 + 2 * (1 - ylo))

    sends = []

    def remote(src, dst, sem, d):
        copy = pltpu.make_async_remote_copy(
            src_ref=src, dst_ref=dst, send_sem=s_sem.at[len(sends)], recv_sem=sem,
            device_id=d, device_id_type=MESH,
        )
        sends.append(copy)
        return copy

    def send(src, dst, sem, d):
        remote(src, dst, sem, d).start()

    def arrived(dst, sem, d):
        pltpu.make_async_remote_copy(
            src_ref=dst, dst_ref=dst, send_sem=s_sem.at[0], recv_sem=sem,
            device_id=d, device_id_type=MESH,
        ).wait_recv()

    base_a = core * 8
    slab_a = base_a + x
    slab_b = base_a + 4 + x

    def rows(zz, part=None):
        if part is None:
            return pl.ds(pl.multiple_of(zz * ROWS, 16), ROWS)
        return pl.ds(pl.multiple_of(zz * ROWS + part * (ROWS // 2), 16), ROWS // 2)

    def piece_a(which):
        return wbuf.at[which, slab_a, rows(z), :]

    def piece_b(which, zz, part=None):
        return wbuf.at[which, slab_b, rows(zz, part), :]

    def bundle(zz, part):
        return wbuf.at[OTH, pl.ds(base_a + 2 * part, 2), rows(zz), :]

    def bundle_whole(zz):
        return wbuf.at[OTH, pl.ds(base_a, 4), rows(zz), :]

    send(piece_b(OWN, z), piece_b(OTH, z), inj_sem.at[1], cross)
    send(piece_a(OWN), piece_a(OTH), inj_sem.at[0], cross)
    half = pl.ds(pl.multiple_of(HALF * mp, 128), HALF)
    other_half = pl.ds(pl.multiple_of(HALF * (1 - mp), 128), HALF)
    for p in range(2):
        dst = xin.at[p, :, half]
        send(f_ref.at[0, mp, p], dst, fx_sem.at[0, p], side)
        send(f_ref.at[0, 1 - mp, p], dst, fx_sem.at[1, p], cross)
    for j in range(1, PIECES):
        send(mstage.at[pl.ds(STRIDE * j, STRIDE)], mrecv.at[j], m_sem, dev(ring(blk, j, BLK), mp))

    def forward_x(ref):
        for k in range(3):
            send(ref, ref, b2_sem.at[k], xdev[k])

    arrived(piece_b(OTH, z), inj_sem.at[1], cross)
    send(piece_b(OTH, z), piece_b(OTH, z), b1_sem.at[0, 0], zplus)
    send(piece_b(OTH, z), piece_b(OTH, z), b1_sem.at[1, 0], zminus)
    arrived(piece_a(OTH), inj_sem.at[0], cross)
    for k in range(3):
        send(piece_a(OTH), piece_a(OTH), a1_sem.at[k], xdev[k])
    forward_x(piece_b(OTH, z))

    def b1_step(step):
        behind, ahead = ring(z, -step, ZS), ring(z, step, ZS)
        if step < 4:
            for direction, zz, d in ((0, behind, zplus), (1, ahead, zminus)):
                ref = piece_b(OTH, zz)
                arrived(ref, b1_sem.at[direction, step - 1], d)
                if step < 3:
                    send(ref, ref, b1_sem.at[direction, step], d)
                else:
                    part = piece_b(OTH, zz, direction)
                    send(part, part, b1_sem.at[direction, step], d)
                forward_x(ref)
        else:
            for direction in range(2):
                ref = piece_b(OTH, behind, direction)
                arrived(ref, b1_sem.at[direction, 3], zplus)
                forward_x(ref)
            whole = wbuf.at[OTH, slab_b]
            send(whole, whole, sib_sem, sibling)

    def a2_start():
        for k in range(3):
            ref = wbuf.at[OTH, base_a + ring(x, -(k + 1), XS), rows(z), :]
            arrived(ref, a1_sem.at[k], xdev[k])
        for part in range(2):
            for direction, d in ((0, zplus), (1, zminus)):
                ref = bundle(z, part)
                send(ref, ref, a2_sem.at[direction, 0, part], d)
        send(bundle_whole(z), bundle_whole(z), sib_sem, sibling)

    def a2_step(step):
        behind, ahead = ring(z, -step, ZS), ring(z, step, ZS)
        if step < 4:
            for part in range(2):
                for direction, zz, d in ((0, behind, zplus), (1, ahead, zminus)):
                    ref = bundle(zz, part)
                    arrived(ref, a2_sem.at[direction, step - 1, part], d)
                    if step < 3 or part == direction:
                        send(ref, ref, a2_sem.at[direction, step, part], d)
            for zz in (behind, ahead):
                send(bundle_whole(zz), bundle_whole(zz), sib_sem, sibling)
        else:
            for direction in range(2):
                arrived(bundle(behind, direction), a2_sem.at[direction, 3, direction], zplus)
            send(bundle_whole(behind), bundle_whole(behind), sib_sem, sibling)

    def b2_finish():
        for k in range(3):
            ref = wbuf.at[OTH, base_a + 4 + ring(x, -(k + 1), XS)]
            arrived(ref, b2_sem.at[k], xdev[k])
            send(ref, ref, sib_sem, sibling)

    def sibling_finish():
        ref = wbuf.at[OTH, pl.ds((1 - core) * 8, 8)]
        arrived(ref, sib_sem, sibling)

    def norm(p):
        def body(i, carry):
            r = pl.ds(pl.multiple_of(i * 64, 64), 64)
            rows_f = xin[p, r, :].astype(F32)
            mean = jnp.mean(rows_f, axis=1, keepdims=True)
            centred = rows_f - mean
            var = jnp.mean(centred * centred, axis=1, keepdims=True)
            nrm[p, r, :] = (centred * lax.rsqrt(var + 1e-05)).astype(BF16)
            return carry

        lax.fori_loop(0, 4, body, 0)
        acc[p] = jnp.dot(xin[p], whz[...], preferred_element_type=F32)

    def project(p, which):
        def body(i, carry):
            w = jnp.concatenate([wbuf[which, 2 * i], wbuf[which, 2 * i + 1]], axis=1)
            r = jnp.dot(nrm[p], w, preferred_element_type=F32)
            qkv[:, pl.ds(pl.multiple_of(256 * i, 256), 256)] = r.astype(BF16)
            return carry

        lax.fori_loop(0, 7, body, 0)
        r = jnp.dot(nrm[p], wbuf[which, 14], preferred_element_type=F32)
        qkv[:, 1792:1920] = r.astype(BF16)

    def attend(p, which):
        def body(i, carry):
            def part(first):
                return qkv[:, pl.ds(pl.multiple_of(first + 128 * i, 128), 128)]

            q, k, v = part(0), part(HALF), part(2 * HALF)
            vo = jnp.concatenate([v, jnp.ones((TOK, 128), BF16)], axis=1)
            outs = []
            for e in range(2):
                keep = low if e == 0 else jnp.logical_not(low)
                qm = jnp.where(keep, q.astype(F32), 0.0).astype(BF16)
                s = lax.dot_general(qm, k, (((1,), (1,)), ((), ())), preferred_element_type=F32)
                s = s - jnp.max(s, axis=1, keepdims=True)
                ex = jnp.exp2(s * EXP_SCALE).astype(BF16)
                o = jnp.dot(ex, vo, preferred_element_type=F32)
                outs.append(o[:, :128] / o[:, 128:])
            joined = jnp.where(low, outs[0], outs[1]).astype(BF16)
            ctx[:, pl.ds(pl.multiple_of(128 * i, 128), 128)] = joined
            return carry

        lax.fori_loop(0, 5, body, 0)
        acc[p] += jnp.dot(ctx[...], wbuf[which, 15, 0:HALF, :], preferred_element_type=F32)

    def selections(r, carry):
        f = iota((FRAME, TOK), 0) - shift
        t = iota((FRAME, TOK), 1) - 16 * r
        hit = (f >= 4 * t) & (f < 4 * t + 4) & (t >= 0) & (t < 16)
        rep[pl.ds(pl.multiple_of(r * FRAME, 16), FRAME), :] = hit.astype(F32).astype(BF16)
        hit = iota((256, LAT), 1) == 16 * r + (iota((256, LAT), 0) & 15)
        fold[r] = hit.astype(F32).astype(BF16)
        return carry

    b1_step(1)
    a2_start()
    b1_step(2)
    lax.fori_loop(0, 8, selections, 0)
    b1_step(3)
    lax.fori_loop(8, 16, selections, 0)
    b1_step(4)
    a2_step(1)
    for h, part in ((0, half), (1, other_half)):
        arrived(xin.at[0, :, part], fx_sem.at[h, 0], side if h == 0 else cross)
    norm(0)
    project(0, OWN)
    a2_step(2)
    attend(0, OWN)
    a2_step(3)
    for h, part in ((0, half), (1, other_half)):
        arrived(xin.at[1, :, part], fx_sem.at[h, 1], side if h == 0 else cross)
    norm(1)
    a2_step(4)
    b2_finish()
    project(1, OWN)
    attend(1, OWN)
    sibling_finish()
    for p in range(2):
        project(p, OTH)
        attend(p, OTH)

    guided = acc[0] + GUIDANCE * (acc[1] - acc[0])
    high = guided.astype(BF16)
    rest = (guided - high.astype(F32)).astype(BF16)
    both = jnp.concatenate([high, rest], axis=1)
    column = ((iota((FRAME, 256), 0) - shift) & 3) == ((iota((FRAME, 256), 1) >> 4) & 3)
    total = jnp.zeros((FRAME, LAT), F32)
    for r in range(16):
        y = jnp.dot(rep[r * FRAME : (r + 1) * FRAME, :], both, preferred_element_type=F32)
        y = jnp.where(column, y, 0.0).astype(BF16)
        total = total + jnp.dot(y, fold[r], preferred_element_type=F32)
    ostage[...] = total

    conditional = None
    for j in range(PIECES):
        src = ostage.at[pl.ds(STRIDE * j, STRIDE)]
        dst = orecv.at[mp, j]
        target = ring(window, j, BLK)
        send(src, dst, o_sem.at[0], dev(target, 1 - mp))
        if j != 2:
            send(src, dst, o_sem.at[1], dev(target, mp))
        else:
            conditional = remote(src, dst, oself_sem, dev(target, mp))

    @pl.when(ylo == 0)
    def _():
        conditional.start()

    @pl.when(ylo == 1)
    def _():
        orecv[mp, 2] = ostage[2 * STRIDE : 3 * STRIDE, :]

    arrived(mrecv.at[pl.ds(1, 4)], m_sem, sibling)
    arrived(orecv.at[mp, pl.ds(0, 4)], o_sem.at[1], sibling)
    arrived(orecv.at[1 - mp], o_sem.at[0], sibling)

    @pl.when(ylo == 0)
    def _():
        arrived(orecv.at[mp, 2], oself_sem, sibling)

    weight = mrecv[0]
    for j in range(1, PIECES):
        weight = weight + mrecv[j]
    for b in range(2):
        value = orecv[b, 0] * mrecv[0]
        for j in range(1, PIECES):
            value = value + orecv[b, j] * mrecv[j]
        out_ref[b] = value / weight

    for copy in sends:
        if copy is conditional:
            @pl.when(ylo == 0)
            def _():
                conditional.wait_send()
        else:
            copy.wait_send()


def shards(features, w_query, w_key, w_value, w_out, w_head, offsets, blend_mask):
    anyspace = pl.BlockSpec(memory_space=pl.ANY)
    return pl.pallas_call(
        kernel,
        out_shape=jax.ShapeDtypeStruct((2, STRIDE, LAT), F32),
        in_specs=[anyspace] * 6 + [pl.BlockSpec(memory_space=pltpu.SMEM), anyspace],
        out_specs=pl.BlockSpec(memory_space=pltpu.VMEM),
        scratch_shapes=[
            pltpu.VMEM((2, SLABS, D, 128), BF16),
            pltpu.VMEM((HALF, D), BF16),
            pltpu.VMEM((D, OUTW), BF16),
            pltpu.VMEM((D, 128), BF16),
            pltpu.VMEM((WINDOW, WINDOW), jnp.int32),
            pltpu.VMEM((2, TOK, D), BF16),
            pltpu.VMEM((2, TOK, D), BF16),
            pltpu.VMEM((TOK, 3 * HALF), BF16),
            pltpu.VMEM((TOK, HALF), BF16),
            pltpu.VMEM((2, TOK, 128), F32),
            pltpu.VMEM((16 * FRAME, TOK), BF16),
            pltpu.VMEM((16, 256, LAT), BF16),
            pltpu.VMEM((FRAME, LAT), F32),
            pltpu.VMEM((PIECES, STRIDE, LAT), F32),
            pltpu.VMEM((FRAME, LAT), F32),
            pltpu.VMEM((2, PIECES, STRIDE, LAT), F32),
            pltpu.SemaphoreType.DMA((20,)),
            pltpu.SemaphoreType.DMA((110,)),
            pltpu.SemaphoreType.DMA((2, 2)),
            pltpu.SemaphoreType.DMA((2,)),
            pltpu.SemaphoreType.DMA((3,)),
            pltpu.SemaphoreType.DMA((2, 4, 2)),
            pltpu.SemaphoreType.DMA((2, 4)),
            pltpu.SemaphoreType.DMA((3,)),
            pltpu.SemaphoreType.DMA,
            pltpu.SemaphoreType.DMA,
            pltpu.SemaphoreType.DMA((2,)),
            pltpu.SemaphoreType.DMA,
        ],
        compiler_params=pltpu.CompilerParams(
            collective_id=0, has_side_effects=True, vmem_limit_bytes=60 * 1024 * 1024
        ),
    )(features, w_query, w_key, w_value, w_out, w_head, offsets, blend_mask)


def solution(mesh):
    return jax.shard_map(
        shards,
        mesh=mesh,
        in_specs=(
            P("blk", None, None, None, "mp"),
            P(None, "mp"),
            P(None, "mp"),
            P(None, "mp"),
            P("mp", None),
            P(),
            P("blk"),
            P("blk", None, None),
        ),
        out_specs=P(None, "blk", None),
        check_vma=False,
    )
```

```python
import jax
import jax.numpy as jnp
from jax import lax
from jax.experimental import pallas as pl
from jax.experimental.pallas import tpu as pltpu
from jax.sharding import PartitionSpec as P

MESH = pl.DeviceIdType.MESH
F32 = jnp.float32
BF16 = jnp.bfloat16

D = 1280
HALF = 640
TOK = 256
OUTW = 64
STRIDE = 16
WINDOW = 64
LAT = 256
FRAME = WINDOW + STRIDE
PIECES = 5
XS, ZS = 4, 8
BLK = 128
ROWS = D // ZS
SLABS = 16
OWN, OTH = 0, 1
EXP_SCALE = 1.4426950408889634 / 8.0
GUIDANCE = 3.0


def dot_t(a, b):
    return lax.dot_general(a, b, (((1,), (1,)), ((), ())), preferred_element_type=F32)


def iota(shape, dim):
    return lax.broadcasted_iota(jnp.int32, shape, dim)


def kernel(
    f_ref, wq_ref, wk_ref, wv_ref, wo_ref, wh_ref, offs_ref, mask_ref, out_ref,
    wbuf, wout, whead, twice, maskv, xin, nrm, qkv, ctx, acc, rep, fold, mstage, mrecv, ostage, orecv,
    ld_sem, s_sem, fx_sem, inj_sem, a1_sem, a2_sem, b1_sem, b2_sem, sib_sem, m_sem, o_sem, oself_sem,
):
    blk = lax.axis_index("blk")
    mp = lax.axis_index("mp")
    core = lax.rem(blk, 2)
    ylo = lax.rem(blk // 2, 2)
    z = lax.rem(blk // 4, ZS)
    x = blk // (4 * ZS)

    def at(xx, zz, yy, cc):
        return ((xx * ZS + zz) * 2 + yy) * 2 + cc

    def dev(b, m):
        return (b, m)

    def ring(v, k, n):
        return lax.rem(v + k + n, n)

    side = dev(at(x, z, 1 - ylo, core), mp)
    cross = dev(at(x, z, 1 - ylo, core), 1 - mp)
    xdev = [dev(at(ring(x, k, XS), z, ylo, core), mp) for k in (1, 2, 3)]
    zplus = dev(at(x, ring(z, 1, ZS), ylo, core), mp)
    zminus = dev(at(x, ring(z, -1, ZS), ylo, core), mp)
    sibling = dev(at(x, z, ylo, 1 - core), mp)
    window = blk + 2 - 4 * ylo

    loads = []

    def load(src, dst):
        copy = pltpu.make_async_copy(src, dst, ld_sem.at[len(loads)])
        copy.start()
        loads.append(copy)
        return copy

    ld_wo = load(wo_ref, wout)
    ld_wh = load(wh_ref, whead)
    ld_mask = load(mask_ref.at[0], maskv)
    ld_w = []
    for m, ref in enumerate((wq_ref, wk_ref, wv_ref)):
        for j in range(5):
            ld_w.append(load(ref.at[:, pl.ds(128 * j, 128)], wbuf.at[OWN, 5 * m + j]))

    barrier = pltpu.get_barrier_semaphore()

    def greet(d):
        pl.semaphore_signal(barrier, inc=1, device_id=d, device_id_type=MESH)

    for d in [side, cross, *xdev, zplus, zminus, sibling]:
        greet(d)

    shift = offs_ref[0] - STRIDE * blk
    ld_wh.wait()
    lane = iota((1, 128), 1)
    low = lane < 64
    twice[0:OUTW, :] = whead[...]
    twice[OUTW:, :] = whead[...]
    ld_wo.wait()
    for r in range(0, HALF, 128):
        prod = dot_t(wout[r : r + 128, :], twice[...])
        head = prod.astype(BF16).astype(F32)
        wbuf[OWN, 15, r : r + 128, :] = jnp.where(low, head, prod - head).astype(BF16)
        wbuf[OWN, 15, HALF + r : HALF + r + 128, :] = jnp.zeros((128, 128), BF16)

    ld_mask.wait()
    widen = (iota((WINDOW, LAT), 0) == (iota((WINDOW, LAT), 1) >> 2)).astype(F32).astype(BF16)
    wide = jnp.dot(maskv[...].astype(F32).astype(BF16), widen, preferred_element_type=F32)
    move = (iota((FRAME, WINDOW), 0) - iota((FRAME, WINDOW), 1) == shift).astype(F32).astype(BF16)
    mstage[...] = jnp.dot(move, wide.astype(BF16), preferred_element_type=F32)
    mrecv[0] = mstage[0:STRIDE, :]

    for copy in ld_w:
        copy.wait()
    pl.semaphore_wait(barrier, 8)

    sends = []

    def remote(src, dst, sem, d):
        copy = pltpu.make_async_remote_copy(
            src_ref=src, dst_ref=dst, send_sem=s_sem.at[len(sends)], recv_sem=sem,
            device_id=d, device_id_type=MESH,
        )
        sends.append(copy)
        return copy

    def send(src, dst, sem, d):
        remote(src, dst, sem, d).start()

    def arrived(dst, sem, d):
        pltpu.make_async_remote_copy(
            src_ref=dst, dst_ref=dst, send_sem=s_sem.at[0], recv_sem=sem,
            device_id=d, device_id_type=MESH,
        ).wait_recv()

    base_a = core * 8
    slab_a = base_a + x
    slab_b = base_a + 4 + x

    def rows(zz, part=None):
        if part is None:
            return pl.ds(pl.multiple_of(zz * ROWS, 16), ROWS)
        return pl.ds(pl.multiple_of(zz * ROWS + part * (ROWS // 2), 16), ROWS // 2)

    def piece_a(which):
        return wbuf.at[which, slab_a, rows(z), :]

    def piece_b(which, zz, part=None):
        return wbuf.at[which, slab_b, rows(zz, part), :]

    def slab_piece(k, zz):
        return wbuf.at[OTH, base_a + ring(x, -k, XS), rows(zz), :]

    def bundle_whole(zz):
        return wbuf.at[OTH, pl.ds(base_a, 4), rows(zz), :]

    send(piece_b(OWN, z), piece_b(OTH, z), inj_sem.at[1], cross)
    send(piece_a(OWN), piece_a(OTH), inj_sem.at[0], cross)
    half = pl.ds(pl.multiple_of(HALF * mp, 128), HALF)
    other_half = pl.ds(pl.multiple_of(HALF * (1 - mp), 128), HALF)
    for p in range(2):
        dst = xin.at[p, :, half]
        send(f_ref.at[0, mp, p], dst, fx_sem.at[0, p], side)
        send(f_ref.at[0, 1 - mp, p], dst, fx_sem.at[1, p], cross)

    def forward_x(ref):
        for k in range(3):
            send(ref, ref, b2_sem.at[k], xdev[k])

    arrived(piece_b(OTH, z), inj_sem.at[1], cross)
    send(piece_b(OTH, z), piece_b(OTH, z), b1_sem.at[0, 0], zplus)
    send(piece_b(OTH, z), piece_b(OTH, z), b1_sem.at[1, 0], zminus)
    arrived(piece_a(OTH), inj_sem.at[0], cross)
    for k in range(3):
        send(piece_a(OTH), piece_a(OTH), a1_sem.at[k], xdev[k])
    for direction, d in ((0, zplus), (1, zminus)):
        send(piece_a(OTH), piece_a(OTH), a2_sem.at[direction, 0, 0], d)
    forward_x(piece_b(OTH, z))

    def b1_step(step):
        behind, ahead = ring(z, -step, ZS), ring(z, step, ZS)
        if step < 4:
            for direction, zz, d in ((0, behind, zplus), (1, ahead, zminus)):
                ref = piece_b(OTH, zz)
                arrived(ref, b1_sem.at[direction, step - 1], d)
                if step < 3:
                    send(ref, ref, b1_sem.at[direction, step], d)
                else:
                    part = piece_b(OTH, zz, direction)
                    send(part, part, b1_sem.at[direction, step], d)
                forward_x(ref)
        else:
            for direction in range(2):
                ref = piece_b(OTH, behind, direction)
                arrived(ref, b1_sem.at[direction, 3], zplus)
                forward_x(ref)
            whole = wbuf.at[OTH, slab_b]
            send(whole, whole, sib_sem, sibling)

    def a2_start():
        for k in (1, 3, 2):
            ref = slab_piece(k, z)
            arrived(ref, a1_sem.at[k - 1], xdev[k - 1])
            for direction, d in ((0, zplus), (1, zminus)):
                send(ref, ref, a2_sem.at[direction, 0, k], d)
        send(bundle_whole(z), bundle_whole(z), sib_sem, sibling)

    def a2_step(step, ks):
        behind, ahead = ring(z, -step, ZS), ring(z, step, ZS)
        for k in ks:
            for direction, zz, d in ((0, behind, zplus), (1, ahead, zminus)):
                last = (k < 2) == (direction == 0)
                if step == 4 and not last:
                    continue
                ref = slab_piece(k, zz)
                arrived(ref, a2_sem.at[direction, step - 1, k], d)
                if step < 3 or (step == 3 and last):
                    send(ref, ref, a2_sem.at[direction, step, k], d)
        if ks[-1] != 0:
            for zz in (behind, ahead) if step < 4 else (behind,):
                send(bundle_whole(zz), bundle_whole(zz), sib_sem, sibling)

    def b2_finish():
        for k in range(3):
            ref = wbuf.at[OTH, base_a + 4 + ring(x, -(k + 1), XS)]
            arrived(ref, b2_sem.at[k], xdev[k])
            send(ref, ref, sib_sem, sibling)

    def sibling_finish():
        ref = wbuf.at[OTH, pl.ds((1 - core) * 8, 8)]
        arrived(ref, sib_sem, sibling)

    def norm(p):
        def body(i, carry):
            r = pl.ds(pl.multiple_of(i * 64, 64), 64)
            rows_f = xin[p, r, :].astype(F32)
            mean = jnp.mean(rows_f, axis=1, keepdims=True)
            centred = rows_f - mean
            var = jnp.mean(centred * centred, axis=1, keepdims=True)
            nrm[p, r, :] = (centred * lax.rsqrt(var + 1e-05)).astype(BF16)
            return carry

        lax.fori_loop(0, 4, body, 0)
        acc[p] = jnp.where(low, dot_t(xin[p], twice[...]), 0.0)

    lane3 = iota((1, 256), 1)

    def project(p, which, first, last):
        for i in range(first, last):
            if i < 7:
                w = jnp.concatenate([wbuf[which, 2 * i], wbuf[which, 2 * i + 1]], axis=1)
            else:
                w = wbuf[which, 14]
            r = jnp.dot(nrm[p], w, preferred_element_type=F32)
            if i < 2:
                r = r * EXP_SCALE
            elif i == 2:
                r = r * jnp.where(lane3 < 128, EXP_SCALE, 1.0)
            qkv[:, 256 * i : 256 * i + r.shape[1]] = r.astype(BF16)

    def attend(p, which, first, last):
        for i in range(first, last):
            q = qkv[:, 128 * i : 128 * i + 128]
            k = qkv[:, HALF + 128 * i : HALF + 128 * i + 128]
            v = qkv[:, 2 * HALF + 128 * i : 2 * HALF + 128 * i + 128]
            vo = jnp.concatenate([v, jnp.ones((TOK, 128), BF16)], axis=1)
            outs = []
            for e in range(2):
                keep = low if e == 0 else jnp.logical_not(low)
                qm = q * keep.astype(F32).astype(BF16)
                s = dot_t(qm, k)
                s = s - jnp.max(s, axis=1, keepdims=True)
                outs.append(jnp.dot(jnp.exp2(s).astype(BF16), vo, preferred_element_type=F32))
            top = jnp.where(low, outs[0][:, :128], outs[1][:, :128])
            bottom = jnp.where(low, outs[0][:, 128:], outs[1][:, 128:])
            ctx[:, 128 * i : 128 * i + 128] = (top / bottom).astype(BF16)
        if last == 5:
            acc[p] += jnp.dot(ctx[...], wbuf[which, 15, 0:HALF, :], preferred_element_type=F32)

    def selections(r, carry):
        f = iota((FRAME, TOK), 0) - shift
        t = iota((FRAME, TOK), 1) - 16 * r
        hit = (f >= 4 * t) & (f < 4 * t + 4) & (t >= 0) & (t < 16)
        rep[pl.ds(pl.multiple_of(r * FRAME, 16), FRAME), :] = hit.astype(F32).astype(BF16)
        hit = iota((256, LAT), 1) == 16 * r + (iota((256, LAT), 0) & 15)
        fold[r] = hit.astype(F32).astype(BF16)
        return carry

    def features_of(p):
        for h, part in ((0, half), (1, other_half)):
            arrived(xin.at[p, :, part], fx_sem.at[h, p], side if h == 0 else cross)

    rest = (1, 3, 2)
    b1_step(1)
    a2_step(1, (0,))
    a2_start()
    lax.fori_loop(0, 8, selections, 0)
    b1_step(2)
    a2_step(2, (0,))
    lax.fori_loop(8, 16, selections, 0)
    a2_step(1, rest)
    b1_step(3)
    features_of(0)
    norm(0)
    a2_step(3, (0,))
    a2_step(2, rest)
    b1_step(4)
    project(0, OWN, 0, 8)
    a2_step(3, rest)
    attend(0, OWN, 0, 5)
    features_of(1)
    norm(1)
    a2_step(4, (0,) + rest)
    project(1, OWN, 0, 8)
    b2_finish()
    attend(1, OWN, 0, 5)
    sibling_finish()
    for p in range(2):
        project(p, OTH, 0, 8)
        attend(p, OTH, 0, 5)

    for j in range(1, PIECES):
        send(mstage.at[pl.ds(STRIDE * j, STRIDE)], mrecv.at[j], m_sem, dev(ring(blk, j, BLK), mp))

    guided = acc[0] + GUIDANCE * (acc[1] - acc[0])
    high = guided.astype(BF16)
    rest = (guided - high.astype(F32)).astype(BF16)
    both = jnp.concatenate([high, rest], axis=1)
    column = ((iota((FRAME, 256), 0) - shift) & 3) == ((iota((FRAME, 256), 1) >> 4) & 3)
    total = jnp.zeros((FRAME, LAT), F32)
    for r in range(16):
        y = jnp.dot(rep[r * FRAME : (r + 1) * FRAME, :], both, preferred_element_type=F32)
        y = jnp.where(column, y, 0.0).astype(BF16)
        total = total + jnp.dot(y, fold[r], preferred_element_type=F32)
    ostage[...] = total

    conditional = None
    for j in range(PIECES):
        src = ostage.at[pl.ds(STRIDE * j, STRIDE)]
        dst = orecv.at[mp, j]
        target = ring(window, j, BLK)
        send(src, dst, o_sem.at[0], dev(target, 1 - mp))
        if j != 2:
            send(src, dst, o_sem.at[1], dev(target, mp))
        else:
            conditional = remote(src, dst, oself_sem, dev(target, mp))

    @pl.when(ylo == 0)
    def _():
        conditional.start()

    @pl.when(ylo == 1)
    def _():
        orecv[mp, 2] = ostage[2 * STRIDE : 3 * STRIDE, :]

    arrived(mrecv.at[pl.ds(1, 4)], m_sem, sibling)
    arrived(orecv.at[mp, pl.ds(0, 4)], o_sem.at[1], sibling)
    arrived(orecv.at[1 - mp], o_sem.at[0], sibling)

    @pl.when(ylo == 0)
    def _():
        arrived(orecv.at[mp, 2], oself_sem, sibling)

    weight = mrecv[0]
    for j in range(1, PIECES):
        weight = weight + mrecv[j]
    for b in range(2):
        value = orecv[b, 0] * mrecv[0]
        for j in range(1, PIECES):
            value = value + orecv[b, j] * mrecv[j]
        out_ref[b] = value / weight

    for copy in sends:
        if copy is conditional:
            @pl.when(ylo == 0)
            def _():
                conditional.wait_send()
        else:
            copy.wait_send()


def shards(features, w_query, w_key, w_value, w_out, w_head, offsets, blend_mask):
    anyspace = pl.BlockSpec(memory_space=pl.ANY)
    return pl.pallas_call(
        kernel,
        out_shape=jax.ShapeDtypeStruct((2, STRIDE, LAT), F32),
        in_specs=[anyspace] * 6 + [pl.BlockSpec(memory_space=pltpu.SMEM), anyspace],
        out_specs=pl.BlockSpec(memory_space=pltpu.VMEM),
        scratch_shapes=[
            pltpu.VMEM((2, SLABS, D, 128), BF16),
            pltpu.VMEM((HALF, D), BF16),
            pltpu.VMEM((OUTW, D), BF16),
            pltpu.VMEM((128, D), BF16),
            pltpu.VMEM((WINDOW, WINDOW), jnp.int32),
            pltpu.VMEM((2, TOK, D), BF16),
            pltpu.VMEM((2, TOK, D), BF16),
            pltpu.VMEM((TOK, 3 * HALF), BF16),
            pltpu.VMEM((TOK, HALF), BF16),
            pltpu.VMEM((2, TOK, 128), F32),
            pltpu.VMEM((16 * FRAME, TOK), BF16),
            pltpu.VMEM((16, 256, LAT), BF16),
            pltpu.VMEM((FRAME, LAT), F32),
            pltpu.VMEM((PIECES, STRIDE, LAT), F32),
            pltpu.VMEM((FRAME, LAT), F32),
            pltpu.VMEM((2, PIECES, STRIDE, LAT), F32),
            pltpu.SemaphoreType.DMA((20,)),
            pltpu.SemaphoreType.DMA((110,)),
            pltpu.SemaphoreType.DMA((2, 2)),
            pltpu.SemaphoreType.DMA((2,)),
            pltpu.SemaphoreType.DMA((3,)),
            pltpu.SemaphoreType.DMA((2, 4, 4)),
            pltpu.SemaphoreType.DMA((2, 4)),
            pltpu.SemaphoreType.DMA((3,)),
            pltpu.SemaphoreType.DMA,
            pltpu.SemaphoreType.DMA,
            pltpu.SemaphoreType.DMA((2,)),
            pltpu.SemaphoreType.DMA,
        ],
        compiler_params=pltpu.CompilerParams(
            collective_id=0, has_side_effects=True, vmem_limit_bytes=60 * 1024 * 1024
        ),
    )(features, w_query, w_key, w_value, w_out, w_head.T, offsets, blend_mask)


def solution(mesh):
    return jax.shard_map(
        shards,
        mesh=mesh,
        in_specs=(
            P("blk", None, None, None, "mp"),
            P(None, "mp"),
            P(None, "mp"),
            P(None, "mp"),
            P("mp", None),
            P(),
            P("blk"),
            P("blk", None, None),
        ),
        out_specs=P(None, "blk", None),
        check_vma=False,
    )
```

```python
import jax
import jax.numpy as jnp
from jax import lax
from jax.experimental import pallas as pl
from jax.experimental.pallas import tpu as pltpu
from jax.sharding import PartitionSpec as P

MESH = pl.DeviceIdType.MESH
F32 = jnp.float32
BF16 = jnp.bfloat16

D = 1280
HALF = 640
TOK = 256
OUTW = 64
STRIDE = 16
WINDOW = 64
LAT = 256
FRAME = WINDOW + STRIDE
PIECES = 5
XS, ZS = 4, 8
BLK = 128
ROWS = D // ZS
SLABS = 16
OWN, OTH = 0, 1
SLAB = ((0, 2), (2, 2), (1, 3), (0, 4), (0, 0), (1, 0), (2, 0), (0, 1), (1, 2), (0, 3), (2, 3), (1, 4), (1, 1), (2, 1), (2, 4))
FIRST_TILES = ((4, 5), (6, 7), (12, 13), (14,))
LAST_TILES = ((0, 8), (1, 9), (2, 10), (3, 11))
CHUNKS = 2
CROWS = TOK // CHUNKS
EXP_SCALE = 1.4426950408889634 / 8.0
GUIDANCE = 3.0


def dot_t(a, b):
    return lax.dot_general(a, b, (((1,), (1,)), ((), ())), preferred_element_type=F32)


def iota(shape, dim):
    return lax.broadcasted_iota(jnp.int32, shape, dim)


def kernel(
    f_ref, wq_ref, wk_ref, wv_ref, wo_ref, wh_ref, offs_ref, mask_ref, out_ref,
    wbuf, wout, whead, twice, maskv, xin, nrm, qkv, ctx, acc, rep, fold, mstage, mrecv, ostage, orecv,
    ld_sem, s_sem, fx_sem, inj_sem, a1_sem, a2_sem, b1_sem, b2_sem, sib_sem, m_sem, o_sem, oself_sem,
):
    blk = lax.axis_index("blk")
    mp = lax.axis_index("mp")
    core = lax.rem(blk, 2)
    ylo = lax.rem(blk // 2, 2)
    z = lax.rem(blk // 4, ZS)
    x = blk // (4 * ZS)

    def at(xx, zz, yy, cc):
        return ((xx * ZS + zz) * 2 + yy) * 2 + cc

    def dev(b, m):
        return (b, m)

    def ring(v, k, n):
        return lax.rem(v + k + n, n)

    side = dev(at(x, z, 1 - ylo, core), mp)
    cross = dev(at(x, z, 1 - ylo, core), 1 - mp)
    xdev = [dev(at(ring(x, k, XS), z, ylo, core), mp) for k in (1, 2, 3)]
    zplus = dev(at(x, ring(z, 1, ZS), ylo, core), mp)
    zminus = dev(at(x, ring(z, -1, ZS), ylo, core), mp)
    sibling = dev(at(x, z, ylo, 1 - core), mp)
    window = blk + 2 - 4 * ylo

    barrier = pltpu.get_barrier_semaphore()

    def greet(d):
        pl.semaphore_signal(barrier, inc=1, device_id=d, device_id_type=MESH)

    for d in [side, cross, *xdev, zplus, zminus, sibling]:
        greet(d)

    loads = []

    def load(src, dst):
        copy = pltpu.make_async_copy(src, dst, ld_sem.at[len(loads)])
        copy.start()
        loads.append(copy)
        return copy

    ld_wo = load(wo_ref, wout)
    ld_wh = load(wh_ref, whead)
    ld_mask = load(mask_ref.at[0], maskv)
    ld_w = []
    for i, (m, j) in enumerate(SLAB):
        ref = (wq_ref, wk_ref, wv_ref)[m]
        ld_w.append(load(ref.at[:, pl.ds(128 * j, 128)], wbuf.at[OWN, i]))

    shift = offs_ref[0] - STRIDE * blk
    ld_wh.wait()
    lane = iota((1, 128), 1)
    low = lane < 64
    twice[0:OUTW, :] = whead[...]
    twice[OUTW:, :] = whead[...]
    ld_wo.wait()
    for r in range(0, HALF, 128):
        prod = dot_t(wout[r : r + 128, :], twice[...])
        head = prod.astype(BF16).astype(F32)
        wbuf[OWN, 15, r : r + 128, :] = jnp.where(low, head, prod - head).astype(BF16)
        wbuf[OWN, 15, HALF + r : HALF + r + 128, :] = jnp.zeros((128, 128), BF16)

    ld_mask.wait()
    widen = (iota((WINDOW, LAT), 0) == (iota((WINDOW, LAT), 1) >> 2)).astype(F32).astype(BF16)
    wide = jnp.dot(maskv[...].astype(F32).astype(BF16), widen, preferred_element_type=F32)
    move = (iota((FRAME, WINDOW), 0) - iota((FRAME, WINDOW), 1) == shift).astype(F32).astype(BF16)
    mstage[...] = jnp.dot(move, wide.astype(BF16), preferred_element_type=F32)
    mrecv[0] = mstage[0:STRIDE, :]

    for copy in ld_w:
        copy.wait()
    pl.semaphore_wait(barrier, 8)

    sends = []

    def remote(src, dst, sem, d):
        copy = pltpu.make_async_remote_copy(
            src_ref=src, dst_ref=dst, send_sem=s_sem.at[len(sends)], recv_sem=sem,
            device_id=d, device_id_type=MESH,
        )
        sends.append(copy)
        return copy

    def send(src, dst, sem, d):
        remote(src, dst, sem, d).start()

    def arrived(dst, sem, d):
        pltpu.make_async_remote_copy(
            src_ref=dst, dst_ref=dst, send_sem=s_sem.at[0], recv_sem=sem,
            device_id=d, device_id_type=MESH,
        ).wait_recv()

    base_a = core * 8
    slab_a = base_a + x
    slab_b = base_a + 4 + x

    def rows(zz, part=None):
        if part is None:
            return pl.ds(pl.multiple_of(zz * ROWS, 16), ROWS)
        return pl.ds(pl.multiple_of(zz * ROWS + part * (ROWS // 2), 16), ROWS // 2)

    def piece_a(which):
        return wbuf.at[which, slab_a, rows(z), :]

    def piece_b(which, zz, part=None):
        return wbuf.at[which, slab_b, rows(zz, part), :]

    def slab_piece(k, zz):
        return wbuf.at[OTH, base_a + ring(x, -k, XS), rows(zz), :]

    send(piece_b(OWN, z), piece_b(OTH, z), inj_sem.at[1], cross)
    send(piece_a(OWN), piece_a(OTH), inj_sem.at[0], cross)
    half = pl.ds(pl.multiple_of(HALF * mp, 128), HALF)
    other_half = pl.ds(pl.multiple_of(HALF * (1 - mp), 128), HALF)
    for p in range(2):
        for i in range(CHUNKS):
            part = pl.ds(CROWS * i, CROWS)
            dst = xin.at[p, part, half]
            send(f_ref.at[0, mp, p, part], dst, fx_sem.at[0, p, i], side)
            send(f_ref.at[0, 1 - mp, p, part], dst, fx_sem.at[1, p, i], cross)

    def forward_x(ref):
        for k in range(3):
            send(ref, ref, b2_sem.at[k], xdev[k])

    arrived(piece_b(OTH, z), inj_sem.at[1], cross)
    send(piece_b(OTH, z), piece_b(OTH, z), b1_sem.at[0, 0], zplus)
    send(piece_b(OTH, z), piece_b(OTH, z), b1_sem.at[1, 0], zminus)
    arrived(piece_a(OTH), inj_sem.at[0], cross)
    for k in range(3):
        send(piece_a(OTH), piece_a(OTH), a1_sem.at[k], xdev[k])
    for direction, d in ((0, zplus), (1, zminus)):
        send(piece_a(OTH), piece_a(OTH), a2_sem.at[direction, 0, 0], d)
    forward_x(piece_b(OTH, z))
    send(piece_a(OTH), piece_a(OTH), sib_sem.at[0], sibling)

    def b1_step(step):
        behind, ahead = ring(z, -step, ZS), ring(z, step, ZS)
        if step < 4:
            for direction, zz, d in ((0, behind, zplus), (1, ahead, zminus)):
                ref = piece_b(OTH, zz)
                arrived(ref, b1_sem.at[direction, step - 1], d)
                if step < 3:
                    send(ref, ref, b1_sem.at[direction, step], d)
                else:
                    part = piece_b(OTH, zz, direction)
                    send(part, part, b1_sem.at[direction, step], d)
                forward_x(ref)
        else:
            for direction in range(2):
                ref = piece_b(OTH, behind, direction)
                arrived(ref, b1_sem.at[direction, 3], zplus)
                forward_x(ref)
            whole = wbuf.at[OTH, slab_b]
            send(whole, whole, sib_sem.at[1], sibling)

    def a2_start():
        for k in (1, 3, 2):
            ref = slab_piece(k, z)
            arrived(ref, a1_sem.at[k - 1], xdev[k - 1])
            for direction, d in ((0, zplus), (1, zminus)):
                send(ref, ref, a2_sem.at[direction, 0, k], d)
            send(ref, ref, sib_sem.at[0], sibling)

    def a2_step(step, ks):
        behind, ahead = ring(z, -step, ZS), ring(z, step, ZS)
        for k in ks:
            for direction, zz, d in ((0, behind, zplus), (1, ahead, zminus)):
                last = (k < 2) == (direction == 0)
                if step == 4 and not last:
                    continue
                ref = slab_piece(k, zz)
                arrived(ref, a2_sem.at[direction, step - 1, k], d)
                if step < 3 or (step == 3 and last):
                    send(ref, ref, a2_sem.at[direction, step, k], d)
                send(ref, ref, sib_sem.at[0], sibling)

    def b2_finish():
        for k in range(3):
            ref = wbuf.at[OTH, base_a + 4 + ring(x, -(k + 1), XS)]
            arrived(ref, b2_sem.at[k], xdev[k])
            send(ref, ref, sib_sem.at[1], sibling)

    def norm(p, i):
        for r in range(CROWS * i, CROWS * (i + 1), 32):
            rows_f = xin[p, r : r + 32, :].astype(F32)
            mean = jnp.mean(rows_f, axis=1, keepdims=True)
            centred = rows_f - mean
            var = jnp.mean(centred * centred, axis=1, keepdims=True)
            nrm[p, r : r + 32, :] = (centred * lax.rsqrt(var + 1e-05)).astype(BF16)
        r = CROWS * i
        acc[p, r : r + CROWS, :] = jnp.where(low, dot_t(xin[p, r : r + CROWS, :], twice[...]), 0.0)

    def project(p, which, tiles, i=None):
        first, count = (0, TOK) if i is None else (CROWS * i, CROWS)
        for tile in tiles:
            parts = [wbuf[which, t] for t in tile]
            w = jnp.concatenate(parts, axis=1) if len(parts) > 1 else parts[0]
            r = jnp.dot(nrm[p, first : first + count, :], w, preferred_element_type=F32)
            for n, t in enumerate(tile):
                m, j = SLAB[t]
                part = r[:, 128 * n : 128 * n + 128]
                if m == 0:
                    part = part * EXP_SCALE
                at_col = 384 * j + 128 * m
                qkv[p, first : first + count, at_col : at_col + 128] = part.astype(BF16)

    def attend(p, which, pairs):
        for i in pairs:
            q, k, v = (qkv[p, :, 384 * i + 128 * m : 384 * i + 128 * m + 128] for m in range(3))
            vo = jnp.concatenate([v, jnp.ones((TOK, 128), BF16)], axis=1)
            outs = []
            for e in range(2):
                keep = low if e == 0 else jnp.logical_not(low)
                qm = q * keep.astype(F32).astype(BF16)
                s = dot_t(qm, k)
                s = s - jnp.max(s, axis=1, keepdims=True)
                outs.append(jnp.dot(jnp.exp2(s).astype(BF16), vo, preferred_element_type=F32))
            top = jnp.where(low, outs[0][:, :128], outs[1][:, :128])
            bottom = jnp.where(low, outs[0][:, 128:], outs[1][:, 128:])
            ctx[p, :, 128 * i : 128 * i + 128] = (top / bottom).astype(BF16)

    def join(p, which):
        acc[p] += jnp.dot(ctx[p], wbuf[which, 15, 0:HALF, :], preferred_element_type=F32)

    def selections(n, carry):
        f = iota((FRAME, TOK), 0) - shift
        for r in (2 * n, 2 * n + 1):
            t = iota((FRAME, TOK), 1) - 16 * r
            hit = (f >= 4 * t) & (f < 4 * t + 4) & (t >= 0) & (t < 16)
            rep[pl.ds(pl.multiple_of(r * FRAME, 16), FRAME), :] = hit.astype(F32).astype(BF16)
        lanes = iota((256, LAT), 0)
        hit = iota((256, LAT), 1) == 32 * n + 16 * (lanes >> 7) + (lanes & 15)
        fold[n] = hit.astype(F32).astype(BF16)
        return carry

    def features_of(p, i):
        for h, part in ((0, half), (1, other_half)):
            arrived(xin.at[p, pl.ds(CROWS * i, CROWS), part], fx_sem.at[h, p, i], side if h == 0 else cross)

    def own_chunk(p, i):
        features_of(p, i)
        norm(p, i)
        project(p, OWN, FIRST_TILES + LAST_TILES, i)

    rest = (1, 3, 2)
    b1_step(1)
    a2_step(1, (0,))
    a2_start()
    lax.fori_loop(0, 8, selections, 0)
    b1_step(2)
    a2_step(2, (0,))
    a2_step(1, rest)
    own_chunk(0, 0)
    b1_step(3)
    a2_step(3, (0,))
    own_chunk(0, 1)
    a2_step(2, rest)
    b1_step(4)
    attend(0, OWN, (0, 1, 2, 3, 4))
    join(0, OWN)
    own_chunk(1, 0)
    a2_step(3, rest)
    own_chunk(1, 1)
    b2_finish()
    attend(1, OWN, (0, 1, 2))
    a2_step(4, (0,) + rest)
    attend(1, OWN, (3, 4))
    join(1, OWN)
    arrived(wbuf.at[OTH, pl.ds((1 - core) * 8 + 4, 4)], sib_sem.at[1], sibling)
    for p in range(2):
        project(p, OTH, FIRST_TILES)
    for p in range(2):
        attend(p, OTH, (0, 1))
    arrived(wbuf.at[OTH, pl.ds((1 - core) * 8, 4)], sib_sem.at[0], sibling)
    for p in range(2):
        project(p, OTH, LAST_TILES)
    for p in range(2):
        attend(p, OTH, (2, 3, 4))
        join(p, OTH)

    for j in range(1, PIECES):
        send(mstage.at[pl.ds(STRIDE * j, STRIDE)], mrecv.at[j], m_sem, dev(ring(blk, j, BLK), mp))

    guided = acc[0] + GUIDANCE * (acc[1] - acc[0])
    guided = guided + pltpu.roll(guided, 64, 1)
    high = guided.astype(BF16).astype(F32)
    both = jnp.where(low, high, guided - high).astype(BF16)
    column = ((iota((FRAME, 256), 0) - shift) & 3) == ((iota((FRAME, 256), 1) >> 4) & 3)
    total = jnp.zeros((FRAME, LAT), F32)
    for n in range(8):
        y = [
            jnp.dot(rep[r * FRAME : (r + 1) * FRAME, :], both, preferred_element_type=F32)
            for r in (2 * n, 2 * n + 1)
        ]
        y = jnp.where(column, jnp.concatenate(y, axis=1), 0.0).astype(BF16)
        total = total + jnp.dot(y, fold[n], preferred_element_type=F32)
    ostage[...] = total

    conditional = None
    for j in range(PIECES):
        src = ostage.at[pl.ds(STRIDE * j, STRIDE)]
        dst = orecv.at[mp, j]
        target = ring(window, j, BLK)
        send(src, dst, o_sem.at[0], dev(target, 1 - mp))
        if j != 2:
            send(src, dst, o_sem.at[1], dev(target, mp))
        else:
            conditional = remote(src, dst, oself_sem, dev(target, mp))

    @pl.when(ylo == 0)
    def _():
        conditional.start()

    @pl.when(ylo == 1)
    def _():
        orecv[mp, 2] = ostage[2 * STRIDE : 3 * STRIDE, :]

    arrived(mrecv.at[pl.ds(1, 4)], m_sem, sibling)
    arrived(orecv.at[mp, pl.ds(0, 4)], o_sem.at[1], sibling)
    arrived(orecv.at[1 - mp], o_sem.at[0], sibling)

    @pl.when(ylo == 0)
    def _():
        arrived(orecv.at[mp, 2], oself_sem, sibling)

    weight = mrecv[0]
    for j in range(1, PIECES):
        weight = weight + mrecv[j]
    for b in range(2):
        value = orecv[b, 0] * mrecv[0]
        for j in range(1, PIECES):
            value = value + orecv[b, j] * mrecv[j]
        out_ref[b] = value / weight

    for copy in sends:
        if copy is conditional:
            @pl.when(ylo == 0)
            def _():
                conditional.wait_send()
        else:
            copy.wait_send()


def shards(features, w_query, w_key, w_value, w_out, w_head, offsets, blend_mask):
    anyspace = pl.BlockSpec(memory_space=pl.ANY)
    return pl.pallas_call(
        kernel,
        out_shape=jax.ShapeDtypeStruct((2, STRIDE, LAT), F32),
        in_specs=[anyspace] * 6 + [pl.BlockSpec(memory_space=pltpu.SMEM), anyspace],
        out_specs=pl.BlockSpec(memory_space=pltpu.VMEM),
        scratch_shapes=[
            pltpu.VMEM((2, SLABS, D, 128), BF16),
            pltpu.VMEM((HALF, D), BF16),
            pltpu.VMEM((OUTW, D), BF16),
            pltpu.VMEM((128, D), BF16),
            pltpu.VMEM((WINDOW, WINDOW), jnp.int32),
            pltpu.VMEM((2, TOK, D), BF16),
            pltpu.VMEM((2, TOK, D), BF16),
            pltpu.VMEM((2, TOK, 3 * HALF), BF16),
            pltpu.VMEM((2, TOK, HALF), BF16),
            pltpu.VMEM((2, TOK, 128), F32),
            pltpu.VMEM((16 * FRAME, TOK), BF16),
            pltpu.VMEM((8, 256, LAT), BF16),
            pltpu.VMEM((FRAME, LAT), F32),
            pltpu.VMEM((PIECES, STRIDE, LAT), F32),
            pltpu.VMEM((FRAME, LAT), F32),
            pltpu.VMEM((2, PIECES, STRIDE, LAT), F32),
            pltpu.SemaphoreType.DMA((20,)),
            pltpu.SemaphoreType.DMA((140,)),
            pltpu.SemaphoreType.DMA((2, 2, CHUNKS)),
            pltpu.SemaphoreType.DMA((2,)),
            pltpu.SemaphoreType.DMA((3,)),
            pltpu.SemaphoreType.DMA((2, 4, 4)),
            pltpu.SemaphoreType.DMA((2, 4)),
            pltpu.SemaphoreType.DMA((3,)),
            pltpu.SemaphoreType.DMA((2,)),
            pltpu.SemaphoreType.DMA,
            pltpu.SemaphoreType.DMA((2,)),
            pltpu.SemaphoreType.DMA,
        ],
        compiler_params=pltpu.CompilerParams(
            collective_id=0, has_side_effects=True, vmem_limit_bytes=60 * 1024 * 1024
        ),
    )(features, w_query, w_key, w_value, w_out, w_head.T, offsets, blend_mask)


def solution(mesh):
    return jax.shard_map(
        shards,
        mesh=mesh,
        in_specs=(
            P("blk", None, None, None, "mp"),
            P(None, "mp"),
            P(None, "mp"),
            P(None, "mp"),
            P("mp", None),
            P(),
            P("blk"),
            P("blk", None, None),
        ),
        out_specs=P(None, "blk", None),
        check_vma=False,
    )
```

```python
import jax
import jax.numpy as jnp
from jax import lax
from jax.experimental import pallas as pl
from jax.experimental.pallas import tpu as pltpu
from jax.sharding import PartitionSpec as P

MESH = pl.DeviceIdType.MESH
F32 = jnp.float32
BF16 = jnp.bfloat16

D = 1280
HALF = 640
TOK = 256
OUTW = 64
STRIDE = 16
WINDOW = 64
LAT = 256
FRAME = WINDOW + STRIDE
PIECES = 5
XS, ZS = 4, 8
BLK = 128
ZP = 4
ROWS = D // ZP
LAST = ZP // 2
SLABS = 16
OWN, OTH = 0, 1
SLAB = ((0, 2), (2, 2), (1, 3), (0, 4), (0, 0), (1, 0), (2, 0), (0, 1), (1, 2), (0, 3), (2, 3), (1, 4), (1, 1), (2, 1), (2, 4))
TILES_B = ((4, 5), (6, 7), (12, 13), (14,))
TILES_A = ((0, 8), (1, 9), (2, 10), (3, 11))
CHUNKS = 2
CROWS = TOK // CHUNKS
EXP_SCALE = 1.4426950408889634 / 8.0
GUIDANCE = 3.0


def dot_t(a, b):
    return lax.dot_general(a, b, (((1,), (1,)), ((), ())), preferred_element_type=F32)


def iota(shape, dim):
    return lax.broadcasted_iota(jnp.int32, shape, dim)


def kernel(
    f_ref, wq_ref, wk_ref, wv_ref, wo_ref, wh_ref, offs_ref, mask_ref, out_ref,
    wbuf, wout, whead, twice, maskv, xin, nrm, qkv, ctx, acc, rep, fold, mstage, mrecv, ostage, orecv,
    ld_sem, s_sem, fx_sem, inj_sem, a1_sem, a2_sem, b1_sem, b2_sem, sib_sem, m_sem, o_sem, oself_sem,
):
    blk = lax.axis_index("blk")
    mp = lax.axis_index("mp")
    core = lax.rem(blk, 2)
    ylo = lax.rem(blk // 2, 2)
    z = lax.rem(blk // 4, ZS)
    x = blk // (4 * ZS)

    def at(xx, zz, yy, cc):
        return ((xx * ZS + zz) * 2 + yy) * 2 + cc

    def dev(b, m):
        return (b, m)

    def ring(v, k, n):
        return lax.rem(v + k + n, n)

    side = dev(at(x, z, 1 - ylo, core), mp)
    cross = dev(at(x, z, 1 - ylo, core), 1 - mp)
    xdev = [dev(at(ring(x, k, XS), z, ylo, core), mp) for k in (1, 2, 3)]
    zplus = dev(at(x, ring(z, 1, ZS), ylo, core), mp)
    zminus = dev(at(x, ring(z, -1, ZS), ylo, core), mp)
    sibling = dev(at(x, z, ylo, 1 - core), mp)
    window = blk + 2 - 4 * ylo

    barrier = pltpu.get_barrier_semaphore()

    low = iota((1, 128), 1) < 64

    def greet(d):
        pl.semaphore_signal(barrier, inc=1, device_id=d, device_id_type=MESH)

    for d in [side, cross, *xdev, zplus, zminus, sibling]:
        greet(d)

    loads = []

    def load(src, dst):
        copy = pltpu.make_async_copy(src, dst, ld_sem.at[len(loads)])
        copy.start()
        loads.append(copy)
        return copy

    ld_wo = load(wo_ref, wout)
    ld_wh = load(wh_ref, whead)
    ld_mask = load(mask_ref.at[0], maskv)
    ld_w = []
    for i, (m, j) in enumerate(SLAB):
        ref = (wq_ref, wk_ref, wv_ref)[m]
        ld_w.append(load(ref.at[:, pl.ds(128 * j, 128)], wbuf.at[OWN, i]))

    pl.semaphore_wait(barrier, 8)

    sends = []

    def remote(src, dst, sem, d):
        copy = pltpu.make_async_remote_copy(
            src_ref=src, dst_ref=dst, send_sem=s_sem.at[len(sends)], recv_sem=sem,
            device_id=d, device_id_type=MESH,
        )
        sends.append(copy)
        return copy

    def send(src, dst, sem, d):
        remote(src, dst, sem, d).start()

    def arrived(dst, sem, d):
        pltpu.make_async_remote_copy(
            src_ref=dst, dst_ref=dst, send_sem=s_sem.at[0], recv_sem=sem,
            device_id=d, device_id_type=MESH,
        ).wait_recv()

    base_a = core * 8
    zp = lax.rem(z, ZP)
    slab_a = base_a + x
    slab_b = base_a + 4 + x

    def rows(zz, part=None):
        if part is None:
            return pl.ds(pl.multiple_of(zz * ROWS, 16), ROWS)
        return pl.ds(pl.multiple_of(zz * ROWS + part * (ROWS // 2), 16), ROWS // 2)

    def piece_a(which):
        return wbuf.at[which, slab_a, rows(zp), :]

    def piece_b(which, zz, part=None):
        return wbuf.at[which, slab_b, rows(zz, part), :]

    def slab_piece(k, zz):
        return wbuf.at[OTH, base_a + ring(x, -k, XS), rows(zz), :]

    def inject(n, sem, i):
        if i < 15:
            m, j = SLAB[i]
            src = (wq_ref, wk_ref, wv_ref)[m].at[rows(zp), pl.ds(128 * j, 128)]
        else:
            src = wbuf.at[OWN, 15, rows(zp), :]

        @pl.when((core == i // 8) & (x == i % 4))
        def _():
            pltpu.make_async_remote_copy(
                src_ref=src, dst_ref=wbuf.at[OTH, i, rows(zp), :], send_sem=s_sem.at[n], recv_sem=sem,
                device_id=cross, device_id_type=MESH,
            ).start()

    remote(piece_a(OTH), piece_a(OTH), inj_sem.at[0], cross)
    remote(piece_b(OTH, zp), piece_b(OTH, zp), inj_sem.at[1], cross)
    for i in (0, 1, 2, 3, 8, 9, 10, 11):
        inject(0, inj_sem.at[0], i)
    for i in (4, 5, 6, 7, 12, 13, 14):
        inject(1, inj_sem.at[1], i)
    half = pl.ds(pl.multiple_of(HALF * mp, 128), HALF)
    other_half = pl.ds(pl.multiple_of(HALF * (1 - mp), 128), HALF)

    def send_features(p, i):
        part = pl.ds(CROWS * i, CROWS)
        dst = xin.at[p, part, half]
        send(f_ref.at[0, mp, p, part], dst, fx_sem.at[0, p, i], side)
        send(f_ref.at[0, 1 - mp, p, part], dst, fx_sem.at[1, p, i], cross)

    send_features(0, 0)
    ld_wh.wait()
    twice[0:OUTW, :] = whead[...]
    twice[OUTW:, :] = whead[...]
    ld_wo.wait()
    for r in range(0, HALF, 128):
        prod = dot_t(wout[r : r + 128, :], twice[...])
        head = prod.astype(BF16).astype(F32)
        wbuf[OWN, 15, r : r + 128, :] = jnp.where(low, head, prod - head).astype(BF16)
        wbuf[OWN, 15, HALF + r : HALF + r + 128, :] = jnp.zeros((128, 128), BF16)

    inject(1, inj_sem.at[1], 15)
    send_features(0, 1)
    for i in range(CHUNKS):
        send_features(1, i)

    shift = offs_ref[0] - STRIDE * blk
    ld_mask.wait()
    widen = (iota((WINDOW, LAT), 0) == (iota((WINDOW, LAT), 1) >> 2)).astype(F32).astype(BF16)
    wide = jnp.dot(maskv[...].astype(F32).astype(BF16), widen, preferred_element_type=F32)
    move = (iota((FRAME, WINDOW), 0) - iota((FRAME, WINDOW), 1) == shift).astype(F32).astype(BF16)
    mstage[...] = jnp.dot(move, wide.astype(BF16), preferred_element_type=F32)
    mrecv[0] = mstage[0:STRIDE, :]


    def forward_x(ref):
        for k in range(3):
            send(ref, ref, b2_sem.at[k], xdev[k])

    arrived(piece_a(OTH), inj_sem.at[0], cross)
    for k in range(3):
        send(piece_a(OTH), piece_a(OTH), a1_sem.at[k], xdev[k])
    for direction, d in ((0, zplus), (1, zminus)):
        send(piece_a(OTH), piece_a(OTH), a2_sem.at[direction, 0, 0], d)
    arrived(piece_b(OTH, zp), inj_sem.at[1], cross)
    send(piece_b(OTH, zp), piece_b(OTH, zp), b1_sem.at[0, 0], zplus)
    send(piece_b(OTH, zp), piece_b(OTH, zp), b1_sem.at[1, 0], zminus)
    forward_x(piece_b(OTH, zp))
    send(piece_a(OTH), piece_a(OTH), sib_sem.at[0], sibling)

    def b1_step(step):
        behind, ahead = ring(zp, -step, ZP), ring(zp, step, ZP)
        if step < LAST:
            for direction, zz, d in ((0, behind, zplus), (1, ahead, zminus)):
                ref = piece_b(OTH, zz)
                arrived(ref, b1_sem.at[direction, step - 1], d)
                if step < LAST - 1:
                    send(ref, ref, b1_sem.at[direction, step], d)
                else:
                    part = piece_b(OTH, zz, direction)
                    send(part, part, b1_sem.at[direction, step], d)
                forward_x(ref)
        else:
            for direction in range(2):
                ref = piece_b(OTH, behind, direction)
                arrived(ref, b1_sem.at[direction, LAST - 1], zplus)
                forward_x(ref)
            whole = wbuf.at[OTH, slab_b]
            send(whole, whole, sib_sem.at[1], sibling)

    def a2_start():
        for k in (1, 3, 2):
            ref = slab_piece(k, zp)
            arrived(ref, a1_sem.at[k - 1], xdev[k - 1])
            for direction, d in ((0, zplus), (1, zminus)):
                send(ref, ref, a2_sem.at[direction, 0, k], d)
            send(ref, ref, sib_sem.at[0], sibling)

    def a2_step(step, ks):
        behind, ahead = ring(zp, -step, ZP), ring(zp, step, ZP)
        for k in ks:
            for direction, zz, d in ((0, behind, zplus), (1, ahead, zminus)):
                last = (k < 2) == (direction == 0)
                if step == LAST and not last:
                    continue
                ref = slab_piece(k, zz)
                arrived(ref, a2_sem.at[direction, step - 1, k], d)
                if step < LAST - 1 or (step == LAST - 1 and last):
                    send(ref, ref, a2_sem.at[direction, step, k], d)
                send(ref, ref, sib_sem.at[0], sibling)

    def b2_finish():
        for k in range(3):
            ref = wbuf.at[OTH, base_a + 4 + ring(x, -(k + 1), XS)]
            arrived(ref, b2_sem.at[k], xdev[k])
            send(ref, ref, sib_sem.at[1], sibling)

    def norm(p, i):
        for r in range(CROWS * i, CROWS * (i + 1), 32):
            rows_f = xin[p, r : r + 32, :].astype(F32)
            mean = jnp.mean(rows_f, axis=1, keepdims=True)
            centred = rows_f - mean
            var = jnp.mean(centred * centred, axis=1, keepdims=True)
            nrm[p, r : r + 32, :] = (centred * lax.rsqrt(var + 1e-05)).astype(BF16)
        r = CROWS * i
        acc[p, r : r + CROWS, :] = jnp.where(low, dot_t(xin[p, r : r + CROWS, :], twice[...]), 0.0)

    def project(p, which, tiles, i=None):
        first, count = (0, TOK) if i is None else (CROWS * i, CROWS)
        for tile in tiles:
            parts = [wbuf[which, t] for t in tile]
            w = jnp.concatenate(parts, axis=1) if len(parts) > 1 else parts[0]
            r = jnp.dot(nrm[p, first : first + count, :], w, preferred_element_type=F32)
            for n, t in enumerate(tile):
                m, j = SLAB[t]
                part = r[:, 128 * n : 128 * n + 128]
                if m == 0:
                    part = part * EXP_SCALE
                at_col = 384 * j + 128 * m
                qkv[p, first : first + count, at_col : at_col + 128] = part.astype(BF16)

    def attend(p, which, pairs):
        for i in pairs:
            q, k, v = (qkv[p, :, 384 * i + 128 * m : 384 * i + 128 * m + 128] for m in range(3))
            vo = jnp.concatenate([v, jnp.ones((TOK, 128), BF16)], axis=1)
            outs = []
            for e in range(2):
                keep = low if e == 0 else jnp.logical_not(low)
                qm = q * keep.astype(F32).astype(BF16)
                s = dot_t(qm, k)
                s = s - jnp.max(s, axis=1, keepdims=True)
                outs.append(jnp.dot(jnp.exp2(s).astype(BF16), vo, preferred_element_type=F32))
            top = jnp.where(low, outs[0][:, :128], outs[1][:, :128])
            bottom = jnp.where(low, outs[0][:, 128:], outs[1][:, 128:])
            ctx[p, :, 128 * i : 128 * i + 128] = (top / bottom).astype(BF16)

    def join(p, which):
        acc[p] += jnp.dot(ctx[p], wbuf[which, 15, 0:HALF, :], preferred_element_type=F32)

    def selections(n, carry):
        f = iota((FRAME, TOK), 0) - shift
        for r in (2 * n, 2 * n + 1):
            t = iota((FRAME, TOK), 1) - 16 * r
            hit = (f >= 4 * t) & (f < 4 * t + 4) & (t >= 0) & (t < 16)
            rep[pl.ds(pl.multiple_of(r * FRAME, 16), FRAME), :] = hit.astype(F32).astype(BF16)
        lanes = iota((256, LAT), 0)
        hit = iota((256, LAT), 1) == 32 * n + 16 * (lanes >> 7) + (lanes & 15)
        fold[n] = hit.astype(F32).astype(BF16)
        return carry

    def features_of(p, i):
        for h, part in ((0, half), (1, other_half)):
            arrived(xin.at[p, pl.ds(CROWS * i, CROWS), part], fx_sem.at[h, p, i], side if h == 0 else cross)

    def own_chunk(p, i):
        features_of(p, i)
        norm(p, i)
        project(p, OWN, TILES_B + TILES_A, i)

    a2_step(1, (0,))
    a2_start()
    b1_step(1)
    lax.fori_loop(0, 8, selections, 0)
    for copy in ld_w:
        copy.wait()
    own_chunk(0, 0)
    a2_step(1, (1, 3))
    own_chunk(0, 1)
    a2_step(1, (2,))
    b1_step(2)
    attend(0, OWN, (0, 1, 2))
    a2_step(2, (0,))
    attend(0, OWN, (3, 4))
    join(0, OWN)
    own_chunk(1, 0)
    a2_step(2, (1, 3, 2))
    own_chunk(1, 1)
    attend(1, OWN, (0, 1))
    b2_finish()
    attend(1, OWN, (2, 3, 4))
    join(1, OWN)
    arrived(wbuf.at[OTH, pl.ds((1 - core) * 8, 4)], sib_sem.at[0], sibling)
    for p in range(2):
        project(p, OTH, TILES_A)
    for p in range(2):
        attend(p, OTH, (2, 3))
    arrived(wbuf.at[OTH, pl.ds((1 - core) * 8 + 4, 4)], sib_sem.at[1], sibling)
    for p in range(2):
        project(p, OTH, TILES_B)
    for p in range(2):
        attend(p, OTH, (0, 1, 4))
        join(p, OTH)

    for j in range(1, PIECES):
        send(mstage.at[pl.ds(STRIDE * j, STRIDE)], mrecv.at[j], m_sem, dev(ring(blk, j, BLK), mp))

    guided = acc[0] + GUIDANCE * (acc[1] - acc[0])
    guided = guided + pltpu.roll(guided, 64, 1)
    high = guided.astype(BF16).astype(F32)
    both = jnp.where(low, high, guided - high).astype(BF16)
    column = ((iota((FRAME, 256), 0) - shift) & 3) == ((iota((FRAME, 256), 1) >> 4) & 3)
    total = jnp.zeros((FRAME, LAT), F32)
    for n in range(8):
        y = [
            jnp.dot(rep[r * FRAME : (r + 1) * FRAME, :], both, preferred_element_type=F32)
            for r in (2 * n, 2 * n + 1)
        ]
        y = jnp.where(column, jnp.concatenate(y, axis=1), 0.0).astype(BF16)
        total = total + jnp.dot(y, fold[n], preferred_element_type=F32)
    ostage[...] = total

    conditional = None
    for j in range(PIECES):
        src = ostage.at[pl.ds(STRIDE * j, STRIDE)]
        dst = orecv.at[mp, j]
        target = ring(window, j, BLK)
        send(src, dst, o_sem.at[0], dev(target, 1 - mp))
        if j != 2:
            send(src, dst, o_sem.at[1], dev(target, mp))
        else:
            conditional = remote(src, dst, oself_sem, dev(target, mp))

    @pl.when(ylo == 0)
    def _():
        conditional.start()

    @pl.when(ylo == 1)
    def _():
        orecv[mp, 2] = ostage[2 * STRIDE : 3 * STRIDE, :]

    arrived(mrecv.at[pl.ds(1, 4)], m_sem, sibling)
    arrived(orecv.at[mp, pl.ds(0, 4)], o_sem.at[1], sibling)
    arrived(orecv.at[1 - mp], o_sem.at[0], sibling)

    @pl.when(ylo == 0)
    def _():
        arrived(orecv.at[mp, 2], oself_sem, sibling)

    weight = mrecv[0]
    for j in range(1, PIECES):
        weight = weight + mrecv[j]
    for b in range(2):
        value = orecv[b, 0] * mrecv[0]
        for j in range(1, PIECES):
            value = value + orecv[b, j] * mrecv[j]
        out_ref[b] = value / weight

    for copy in sends:
        if copy is conditional:
            @pl.when(ylo == 0)
            def _():
                conditional.wait_send()
        else:
            copy.wait_send()


def shards(features, w_query, w_key, w_value, w_out, w_head, offsets, blend_mask):
    anyspace = pl.BlockSpec(memory_space=pl.ANY)
    return pl.pallas_call(
        kernel,
        out_shape=jax.ShapeDtypeStruct((2, STRIDE, LAT), F32),
        in_specs=[anyspace] * 6 + [pl.BlockSpec(memory_space=pltpu.SMEM), anyspace],
        out_specs=pl.BlockSpec(memory_space=pltpu.VMEM),
        scratch_shapes=[
            pltpu.VMEM((2, SLABS, D, 128), BF16),
            pltpu.VMEM((HALF, D), BF16),
            pltpu.VMEM((OUTW, D), BF16),
            pltpu.VMEM((128, D), BF16),
            pltpu.VMEM((WINDOW, WINDOW), jnp.int32),
            pltpu.VMEM((2, TOK, D), BF16),
            pltpu.VMEM((2, TOK, D), BF16),
            pltpu.VMEM((2, TOK, 3 * HALF), BF16),
            pltpu.VMEM((2, TOK, HALF), BF16),
            pltpu.VMEM((2, TOK, 128), F32),
            pltpu.VMEM((16 * FRAME, TOK), BF16),
            pltpu.VMEM((8, 256, LAT), BF16),
            pltpu.VMEM((FRAME, LAT), F32),
            pltpu.VMEM((PIECES, STRIDE, LAT), F32),
            pltpu.VMEM((FRAME, LAT), F32),
            pltpu.VMEM((2, PIECES, STRIDE, LAT), F32),
            pltpu.SemaphoreType.DMA((20,)),
            pltpu.SemaphoreType.DMA((140,)),
            pltpu.SemaphoreType.DMA((2, 2, CHUNKS)),
            pltpu.SemaphoreType.DMA((2,)),
            pltpu.SemaphoreType.DMA((3,)),
            pltpu.SemaphoreType.DMA((2, 4, 4)),
            pltpu.SemaphoreType.DMA((2, 4)),
            pltpu.SemaphoreType.DMA((3,)),
            pltpu.SemaphoreType.DMA((2,)),
            pltpu.SemaphoreType.DMA,
            pltpu.SemaphoreType.DMA((2,)),
            pltpu.SemaphoreType.DMA,
        ],
        compiler_params=pltpu.CompilerParams(
            collective_id=0, has_side_effects=True, vmem_limit_bytes=60 * 1024 * 1024
        ),
    )(features, w_query, w_key, w_value, w_out, w_head.T, offsets, blend_mask)


def solution(mesh):
    return jax.shard_map(
        shards,
        mesh=mesh,
        in_specs=(
            P("blk", None, None, None, "mp"),
            P(None, "mp"),
            P(None, "mp"),
            P(None, "mp"),
            P("mp", None),
            P(),
            P("blk"),
            P("blk", None, None),
        ),
        out_specs=P(None, "blk", None),
        check_vma=False,
    )
```

```python
import jax
import jax.numpy as jnp
from jax import lax
from jax.experimental import pallas as pl
from jax.experimental.pallas import tpu as pltpu
from jax.sharding import PartitionSpec as P

MESH = pl.DeviceIdType.MESH
F32 = jnp.float32
BF16 = jnp.bfloat16

D = 1280
HALF = 640
TOK = 256
OUTW = 64
STRIDE = 16
WINDOW = 64
LAT = 256
FRAME = WINDOW + STRIDE
PIECES = 5
XS, ZS = 4, 8
BLK = 128
ZP = 4
ROWS = D // ZP
LAST = ZP // 2
SLABS = 16
OWN, OTH = 0, 1
SLAB = ((0, 2), (2, 2), (1, 3), (0, 4), (0, 0), (1, 0), (2, 0), (0, 1), (1, 2), (0, 3), (2, 3), (1, 4), (1, 1), (2, 1), (2, 4))
TILES_B = ((4, 5), (6, 7), (12, 13), (14,))
TILES_A = ((0, 8), (1, 9), (2, 10), (3, 11))
CHUNKS = 2
CROWS = TOK // CHUNKS
EXP_SCALE = 1.4426950408889634 / 8.0
GUIDANCE = 3.0


def dot_t(a, b):
    return lax.dot_general(a, b, (((1,), (1,)), ((), ())), preferred_element_type=F32)


def iota(shape, dim):
    return lax.broadcasted_iota(jnp.int32, shape, dim)


def kernel(
    f_ref, wq_ref, wk_ref, wv_ref, wo_ref, wh_ref, offs_ref, mask_ref, out_ref,
    wbuf, wout, whead, twice, maskv, xin, nrm, qkv, ctx, acc, rep, fold, mstage, mrecv, ostage, orecv,
    ld_sem, s_sem, fx_sem, inj_sem, a1_sem, a2_sem, b1_sem, b2_sem, sib_sem, m_sem, o_sem, oself_sem,
):
    blk = lax.axis_index("blk")
    mp = lax.axis_index("mp")
    core = lax.rem(blk, 2)
    ylo = lax.rem(blk // 2, 2)
    z = lax.rem(blk // 4, ZS)
    x = blk // (4 * ZS)

    def at(xx, zz, yy, cc):
        return ((xx * ZS + zz) * 2 + yy) * 2 + cc

    def dev(b, m):
        return (b, m)

    def ring(v, k, n):
        return lax.rem(v + k + n, n)

    side = dev(at(x, z, 1 - ylo, core), mp)
    cross = dev(at(x, z, 1 - ylo, core), 1 - mp)
    xdev = [dev(at(ring(x, k, XS), z, ylo, core), mp) for k in (1, 2, 3)]
    zplus = dev(at(x, ring(z, 1, ZS), ylo, core), mp)
    zminus = dev(at(x, ring(z, -1, ZS), ylo, core), mp)
    sibling = dev(at(x, z, ylo, 1 - core), mp)
    window = blk + 2 - 4 * ylo

    barrier = pltpu.get_barrier_semaphore()

    low = iota((1, 128), 1) < 64

    def greet(d):
        pl.semaphore_signal(barrier, inc=1, device_id=d, device_id_type=MESH)

    for d in [side, cross, *xdev, zplus, zminus, sibling]:
        greet(d)

    loads = []

    def load(src, dst):
        copy = pltpu.make_async_copy(src, dst, ld_sem.at[len(loads)])
        copy.start()
        loads.append(copy)
        return copy

    ld_wo = load(wo_ref, wout)
    ld_wh = load(wh_ref, whead)
    ld_mask = load(mask_ref.at[0], maskv)
    ld_w = []
    for i, (m, j) in enumerate(SLAB):
        ref = (wq_ref, wk_ref, wv_ref)[m]
        ld_w.append(load(ref.at[:, pl.ds(128 * j, 128)], wbuf.at[OWN, i]))

    pl.semaphore_wait(barrier, 8)

    sends = []

    def remote(src, dst, sem, d):
        copy = pltpu.make_async_remote_copy(
            src_ref=src, dst_ref=dst, send_sem=s_sem.at[len(sends)], recv_sem=sem,
            device_id=d, device_id_type=MESH,
        )
        sends.append(copy)
        return copy

    def send(src, dst, sem, d):
        remote(src, dst, sem, d).start()

    def arrived(dst, sem, d):
        pltpu.make_async_remote_copy(
            src_ref=dst, dst_ref=dst, send_sem=s_sem.at[0], recv_sem=sem,
            device_id=d, device_id_type=MESH,
        ).wait_recv()

    base_a = core * 8
    zp = lax.rem(z, ZP)
    slab_a = base_a + x
    slab_b = base_a + 4 + x

    def rows(zz, part=None):
        if part is None:
            return pl.ds(pl.multiple_of(zz * ROWS, 16), ROWS)
        return pl.ds(pl.multiple_of(zz * ROWS + part * (ROWS // 2), 16), ROWS // 2)

    def piece_a(which):
        return wbuf.at[which, slab_a, rows(zp), :]

    def piece_b(which, zz, part=None):
        return wbuf.at[which, slab_b, rows(zz, part), :]

    def slab_piece(k, zz):
        return wbuf.at[OTH, base_a + ring(x, -k, XS), rows(zz), :]

    def inject(n, sem, i):
        if i < 15:
            m, j = SLAB[i]
            src = (wq_ref, wk_ref, wv_ref)[m].at[rows(zp), pl.ds(128 * j, 128)]
        else:
            src = wbuf.at[OWN, 15, rows(zp), :]

        @pl.when((core == i // 8) & (x == i % 4))
        def _():
            pltpu.make_async_remote_copy(
                src_ref=src, dst_ref=wbuf.at[OTH, i, rows(zp), :], send_sem=s_sem.at[n], recv_sem=sem,
                device_id=cross, device_id_type=MESH,
            ).start()

    remote(piece_a(OTH), piece_a(OTH), inj_sem.at[0], cross)
    remote(piece_b(OTH, zp), piece_b(OTH, zp), inj_sem.at[1], cross)
    for i in (0, 1, 2, 3, 8, 9, 10, 11):
        inject(0, inj_sem.at[0], i)
    for i in (4, 5, 6, 7, 12, 13, 14):
        inject(1, inj_sem.at[1], i)
    half = pl.ds(pl.multiple_of(HALF * mp, 128), HALF)
    other_half = pl.ds(pl.multiple_of(HALF * (1 - mp), 128), HALF)

    def send_features(p, i):
        part = pl.ds(CROWS * i, CROWS)
        dst = xin.at[p, part, half]
        send(f_ref.at[0, mp, p, part], dst, fx_sem.at[0, p, i], side)
        send(f_ref.at[0, 1 - mp, p, part], dst, fx_sem.at[1, p, i], cross)

    send_features(0, 0)
    ld_wh.wait()
    twice[0:OUTW, :] = whead[...]
    twice[OUTW:, :] = whead[...]
    ld_wo.wait()
    for r in range(0, HALF, 128):
        prod = dot_t(wout[r : r + 128, :], twice[...])
        head = prod.astype(BF16).astype(F32)
        wbuf[OWN, 15, r : r + 128, :] = jnp.where(low, head, prod - head).astype(BF16)
        wbuf[OWN, 15, HALF + r : HALF + r + 128, :] = jnp.zeros((128, 128), BF16)

    inject(1, inj_sem.at[1], 15)
    send_features(0, 1)
    for i in range(CHUNKS):
        send_features(1, i)

    shift = offs_ref[0] - STRIDE * blk
    ld_mask.wait()
    widen = (iota((WINDOW, LAT), 0) == (iota((WINDOW, LAT), 1) >> 2)).astype(F32).astype(BF16)
    wide = jnp.dot(maskv[...].astype(F32).astype(BF16), widen, preferred_element_type=F32)
    move = (iota((FRAME, WINDOW), 0) - iota((FRAME, WINDOW), 1) == shift).astype(F32).astype(BF16)
    mstage[...] = jnp.dot(move, wide.astype(BF16), preferred_element_type=F32)
    mrecv[0] = mstage[0:STRIDE, :]


    def forward_x(ref, last=0):
        for k in (1, 0, 2):
            send(ref, ref, b2_sem.at[k, last], xdev[k])

    arrived(piece_a(OTH), inj_sem.at[0], cross)
    for k in range(3):
        send(piece_a(OTH), piece_a(OTH), a1_sem.at[k], xdev[k])
    for direction, d in ((0, zplus), (1, zminus)):
        send(piece_a(OTH), piece_a(OTH), a2_sem.at[direction, 0, 0], d)
    arrived(piece_b(OTH, zp), inj_sem.at[1], cross)
    send(piece_b(OTH, zp), piece_b(OTH, zp), b1_sem.at[0, 0], zplus)
    send(piece_b(OTH, zp), piece_b(OTH, zp), b1_sem.at[1, 0], zminus)
    forward_x(piece_b(OTH, zp))
    send(piece_a(OTH), piece_a(OTH), sib_sem.at[0], sibling)
    send(piece_b(OTH, zp), piece_b(OTH, zp), sib_sem.at[1], sibling)

    def b1_step(step):
        behind, ahead = ring(zp, -step, ZP), ring(zp, step, ZP)
        if step < LAST:
            for direction, zz, d in ((0, behind, zplus), (1, ahead, zminus)):
                ref = piece_b(OTH, zz)
                arrived(ref, b1_sem.at[direction, step - 1], d)
                if step < LAST - 1:
                    send(ref, ref, b1_sem.at[direction, step], d)
                else:
                    part = piece_b(OTH, zz, direction)
                    send(part, part, b1_sem.at[direction, step], d)
                forward_x(ref)
                send(ref, ref, sib_sem.at[1], sibling)
        else:
            for direction in range(2):
                ref = piece_b(OTH, behind, direction)
                arrived(ref, b1_sem.at[direction, LAST - 1], zplus)
                forward_x(ref, 1)
            send(piece_b(OTH, behind), piece_b(OTH, behind), sib_sem.at[1], sibling)

    def a2_start():
        for k in (1, 3, 2):
            ref = slab_piece(k, zp)
            arrived(ref, a1_sem.at[k - 1], xdev[k - 1])
            for direction, d in ((0, zplus), (1, zminus)):
                send(ref, ref, a2_sem.at[direction, 0, k], d)
            send(ref, ref, sib_sem.at[0], sibling)

    def a2_step(step, ks):
        behind, ahead = ring(zp, -step, ZP), ring(zp, step, ZP)
        for k in ks:
            for direction, zz, d in ((0, behind, zplus), (1, ahead, zminus)):
                last = (k < 2) == (direction == 0)
                if step == LAST and not last:
                    continue
                ref = slab_piece(k, zz)
                arrived(ref, a2_sem.at[direction, step - 1, k], d)
                if step < LAST - 1 or (step == LAST - 1 and last):
                    send(ref, ref, a2_sem.at[direction, step, k], d)
                send(ref, ref, sib_sem.at[0], sibling)

    def b2_slab(k, zz):
        return wbuf.at[OTH, base_a + 4 + ring(x, -(k + 1), XS), rows(zz), :]

    def b2_first():
        for k in range(3):
            near = [b2_slab(k, ring(zp, n, ZP)) for n in (0, 1, 3)]
            whole = wbuf.at[OTH, base_a + 4 + ring(x, -(k + 1), XS), pl.ds(0, 3 * ROWS), :]
            arrived(whole, b2_sem.at[k, 0], xdev[k])
            for ref in near:
                send(ref, ref, sib_sem.at[1], sibling)

    def b2_last():
        for k in (0, 2, 1):
            ref = b2_slab(k, ring(zp, 2, ZP))
            arrived(ref, b2_sem.at[k, 1], xdev[k])
            send(ref, ref, sib_sem.at[1], sibling)

    def norm(p, i):
        for r in range(CROWS * i, CROWS * (i + 1), 32):
            rows_f = xin[p, r : r + 32, :].astype(F32)
            mean = jnp.mean(rows_f, axis=1, keepdims=True)
            centred = rows_f - mean
            var = jnp.mean(centred * centred, axis=1, keepdims=True)
            nrm[p, r : r + 32, :] = (centred * lax.rsqrt(var + 1e-05)).astype(BF16)
        r = CROWS * i
        acc[p, r : r + CROWS, :] = jnp.where(low, dot_t(xin[p, r : r + CROWS, :], twice[...]), 0.0)

    def project(p, which, tiles, i=None):
        first, count = (0, TOK) if i is None else (CROWS * i, CROWS)
        for tile in tiles:
            parts = [wbuf[which, t] for t in tile]
            w = jnp.concatenate(parts, axis=1) if len(parts) > 1 else parts[0]
            r = jnp.dot(nrm[p, first : first + count, :], w, preferred_element_type=F32)
            for n, t in enumerate(tile):
                m, j = SLAB[t]
                part = r[:, 128 * n : 128 * n + 128]
                if m == 0:
                    part = part * EXP_SCALE
                at_col = 384 * j + 128 * m
                qkv[p, first : first + count, at_col : at_col + 128] = part.astype(BF16)

    def attend(p, which, pairs):
        for i in pairs:
            q, k, v = (qkv[p, :, 384 * i + 128 * m : 384 * i + 128 * m + 128] for m in range(3))
            vo = jnp.concatenate([v, jnp.ones((TOK, 128), BF16)], axis=1)
            outs = []
            for e in range(2):
                keep = low if e == 0 else jnp.logical_not(low)
                qm = q * keep.astype(F32).astype(BF16)
                s = dot_t(qm, k)
                s = s - jnp.max(s, axis=1, keepdims=True)
                outs.append(jnp.dot(jnp.exp2(s).astype(BF16), vo, preferred_element_type=F32))
            top = jnp.where(low, outs[0][:, :128], outs[1][:, :128])
            bottom = jnp.where(low, outs[0][:, 128:], outs[1][:, 128:])
            ctx[p, :, 128 * i : 128 * i + 128] = (top / bottom).astype(BF16)

    def join(p, which):
        acc[p] += jnp.dot(ctx[p], wbuf[which, 15, 0:HALF, :], preferred_element_type=F32)

    def selections(n, carry):
        f = iota((FRAME, TOK), 0) - shift
        for r in (2 * n, 2 * n + 1):
            t = iota((FRAME, TOK), 1) - 16 * r
            hit = (f >= 4 * t) & (f < 4 * t + 4) & (t >= 0) & (t < 16)
            rep[pl.ds(pl.multiple_of(r * FRAME, 16), FRAME), :] = hit.astype(F32).astype(BF16)
        lanes = iota((256, LAT), 0)
        hit = iota((256, LAT), 1) == 32 * n + 16 * (lanes >> 7) + (lanes & 15)
        fold[n] = hit.astype(F32).astype(BF16)
        return carry

    def features_of(p, i):
        for h, part in ((0, half), (1, other_half)):
            arrived(xin.at[p, pl.ds(CROWS * i, CROWS), part], fx_sem.at[h, p, i], side if h == 0 else cross)

    def own_chunk(p, i):
        features_of(p, i)
        norm(p, i)
        project(p, OWN, TILES_B + TILES_A, i)

    a2_step(1, (0,))
    a2_start()
    b1_step(1)
    lax.fori_loop(0, 8, selections, 0)
    for copy in ld_w:
        copy.wait()
    own_chunk(0, 0)
    a2_step(1, (1, 3))
    own_chunk(0, 1)
    a2_step(1, (2,))
    b1_step(2)
    attend(0, OWN, (0, 1, 2))
    a2_step(2, (0,))
    attend(0, OWN, (3, 4))
    join(0, OWN)
    own_chunk(1, 0)
    a2_step(2, (1, 3, 2))
    b2_first()
    own_chunk(1, 1)
    attend(1, OWN, (0, 1, 2, 3, 4))
    join(1, OWN)
    b2_last()
    arrived(wbuf.at[OTH, pl.ds((1 - core) * 8, 4)], sib_sem.at[0], sibling)
    for p in range(2):
        project(p, OTH, TILES_A)
    for p in range(2):
        attend(p, OTH, (2, 3))
    arrived(wbuf.at[OTH, pl.ds((1 - core) * 8 + 4, 4)], sib_sem.at[1], sibling)
    for p in range(2):
        project(p, OTH, TILES_B)
    for p in range(2):
        attend(p, OTH, (0, 1, 4))
        join(p, OTH)

    for j in range(1, PIECES):
        send(mstage.at[pl.ds(STRIDE * j, STRIDE)], mrecv.at[j], m_sem, dev(ring(blk, j, BLK), mp))

    guided = acc[0] + GUIDANCE * (acc[1] - acc[0])
    guided = guided + pltpu.roll(guided, 64, 1)
    high = guided.astype(BF16).astype(F32)
    both = jnp.where(low, high, guided - high).astype(BF16)
    column = ((iota((FRAME, 256), 0) - shift) & 3) == ((iota((FRAME, 256), 1) >> 4) & 3)
    total = jnp.zeros((FRAME, LAT), F32)
    for n in range(8):
        y = [
            jnp.dot(rep[r * FRAME : (r + 1) * FRAME, :], both, preferred_element_type=F32)
            for r in (2 * n, 2 * n + 1)
        ]
        y = jnp.where(column, jnp.concatenate(y, axis=1), 0.0).astype(BF16)
        total = total + jnp.dot(y, fold[n], preferred_element_type=F32)
    ostage[...] = total

    conditional = None
    for j in range(PIECES):
        src = ostage.at[pl.ds(STRIDE * j, STRIDE)]
        dst = orecv.at[mp, j]
        target = ring(window, j, BLK)
        send(src, dst, o_sem.at[0], dev(target, 1 - mp))
        if j != 2:
            send(src, dst, o_sem.at[1], dev(target, mp))
        else:
            conditional = remote(src, dst, oself_sem, dev(target, mp))

    @pl.when(ylo == 0)
    def _():
        conditional.start()

    @pl.when(ylo == 1)
    def _():
        orecv[mp, 2] = ostage[2 * STRIDE : 3 * STRIDE, :]

    arrived(mrecv.at[pl.ds(1, 4)], m_sem, sibling)
    arrived(orecv.at[mp, pl.ds(0, 4)], o_sem.at[1], sibling)
    arrived(orecv.at[1 - mp], o_sem.at[0], sibling)

    @pl.when(ylo == 0)
    def _():
        arrived(orecv.at[mp, 2], oself_sem, sibling)

    weight = mrecv[0]
    for j in range(1, PIECES):
        weight = weight + mrecv[j]
    for b in range(2):
        value = orecv[b, 0] * mrecv[0]
        for j in range(1, PIECES):
            value = value + orecv[b, j] * mrecv[j]
        out_ref[b] = value / weight

    for copy in sends:
        if copy is conditional:
            @pl.when(ylo == 0)
            def _():
                conditional.wait_send()
        else:
            copy.wait_send()


def shards(features, w_query, w_key, w_value, w_out, w_head, offsets, blend_mask):
    anyspace = pl.BlockSpec(memory_space=pl.ANY)
    return pl.pallas_call(
        kernel,
        out_shape=jax.ShapeDtypeStruct((2, STRIDE, LAT), F32),
        in_specs=[anyspace] * 6 + [pl.BlockSpec(memory_space=pltpu.SMEM), anyspace],
        out_specs=pl.BlockSpec(memory_space=pltpu.VMEM),
        scratch_shapes=[
            pltpu.VMEM((2, SLABS, D, 128), BF16),
            pltpu.VMEM((HALF, D), BF16),
            pltpu.VMEM((OUTW, D), BF16),
            pltpu.VMEM((128, D), BF16),
            pltpu.VMEM((WINDOW, WINDOW), jnp.int32),
            pltpu.VMEM((2, TOK, D), BF16),
            pltpu.VMEM((2, TOK, D), BF16),
            pltpu.VMEM((2, TOK, 3 * HALF), BF16),
            pltpu.VMEM((2, TOK, HALF), BF16),
            pltpu.VMEM((2, TOK, 128), F32),
            pltpu.VMEM((16 * FRAME, TOK), BF16),
            pltpu.VMEM((8, 256, LAT), BF16),
            pltpu.VMEM((FRAME, LAT), F32),
            pltpu.VMEM((PIECES, STRIDE, LAT), F32),
            pltpu.VMEM((FRAME, LAT), F32),
            pltpu.VMEM((2, PIECES, STRIDE, LAT), F32),
            pltpu.SemaphoreType.DMA((20,)),
            pltpu.SemaphoreType.DMA((140,)),
            pltpu.SemaphoreType.DMA((2, 2, CHUNKS)),
            pltpu.SemaphoreType.DMA((2,)),
            pltpu.SemaphoreType.DMA((3,)),
            pltpu.SemaphoreType.DMA((2, 4, 4)),
            pltpu.SemaphoreType.DMA((2, 4)),
            pltpu.SemaphoreType.DMA((3, 2)),
            pltpu.SemaphoreType.DMA((2,)),
            pltpu.SemaphoreType.DMA,
            pltpu.SemaphoreType.DMA((2,)),
            pltpu.SemaphoreType.DMA,
        ],
        compiler_params=pltpu.CompilerParams(
            collective_id=0, has_side_effects=True, vmem_limit_bytes=60 * 1024 * 1024
        ),
    )(features, w_query, w_key, w_value, w_out, w_head.T, offsets, blend_mask)


def solution(mesh):
    return jax.shard_map(
        shards,
        mesh=mesh,
        in_specs=(
            P("blk", None, None, None, "mp"),
            P(None, "mp"),
            P(None, "mp"),
            P(None, "mp"),
            P("mp", None),
            P(),
            P("blk"),
            P("blk", None, None),
        ),
        out_specs=P(None, "blk", None),
        check_vma=False,
    )
```
